512 devices in a mesh: groups: 2 (over y), dp: 128 (over z, x), tensor: 2 (over core).
Axes of the slice: x: 8, y: 2, z: 16, core: 2. Of those that a mesh axis runs over, the one named last changes fastest.
The devices are a block of a 8x8x16 slice.
Arguments:
- cache_keys: bfloat16 [256, 2048, 1024], P(('groups', 'dp'), None, 'tensor'), parts along dimension 0, may hold values from -32 to 32
- cache_values: bfloat16 [256, 2048, 1024], P(('groups', 'dp'), None, 'tensor'), parts along dimension 0, may hold values from -6 to 6
- lengths: int32 [256], P(('groups', 'dp')), parts along dimension 0, may hold values from 512 to 2048
- parent_scores: float32 [256], P(('groups', 'dp')), parts along dimension 0, may hold values from -6 to 0
- parents: int32 [256], P(('groups', 'dp')), parts along dimension 0, may hold values from 0 to 127, as said below
- queries: bfloat16 [256, 4, 8192], P(('groups', 'dp'), None, 'tensor'), parts along dimension 0, may hold values from -32 to 32
- new_keys: bfloat16 [256, 4, 1024], P(('groups', 'dp'), None, 'tensor'), parts along dimension 0, may hold values from -9 to 9
- new_values: bfloat16 [256, 4, 1024], P(('groups', 'dp'), None, 'tensor'), parts along dimension 0, may hold values from -6 to 6
- reward_weight: bfloat16 [8192], P('tensor'), may hold values from -3 to 3
Outputs:
- attended: bfloat16 [256, 4, 8192], P(('groups', 'dp'), None, 'tensor'), parts along dimension 0
- scores: float32 [256], P(('groups', 'dp')), parts along dimension 0
The draws below stay inside these ranges and needn't reach their ends.
There are 2 independent parts, one for each index of `groups`. The reference program is written for one: setup_inputs(seed, part) draws one part's arguments, and reference() takes and returns one part's arrays. A program takes and returns all parts, laid end to end along the dimension named above; an argument that names none is the same for every part. Nothing has to cross between parts.
Inputs may be any that keep to these rules, and one draw needn't show every extreme that they name: `parents`: each old beam is continued by at most 2 new slots; in every draw some old beams are continued by exactly 2 and others by none.
All inputs are finite; a program needn't handle non-finite values.
Results may differ from the reference program's by a relative error of at most 0.0056.
Values may be sent and summed in bfloat16 or wider, within the bound.
No kernel may reach another device: no remote copies, remote signals or barrier semaphores. Data moves between devices by JAX's collectives and lax.ppermute only.
A program may use at most 64 MiB of HBM per device.

```python
import jax
import jax.numpy as jnp
from jax import lax

QH = 64
KVH = 8
HD = 128
CTX = 2048
STEPS = 4
BEAMS = 128


def parent_table(key):
    base = jax.random.fold_in(key, 7001)
    key_order, key_shuffle = jax.random.split(base, 2)
    order = jax.random.permutation(key_order, BEAMS)
    ranked = jnp.arange(BEAMS)
    by_rank = jnp.where(ranked < BEAMS // 4, 2, jnp.where(ranked < 3 * (BEAMS // 4), 1, 0)).astype(jnp.int32)
    counts = jnp.zeros((BEAMS,), jnp.int32).at[order].set(by_rank)
    listed = jnp.repeat(jnp.arange(BEAMS, dtype=jnp.int32), counts, total_repeat_length=BEAMS)
    shuffle = jax.random.permutation(key_shuffle, BEAMS)
    listed = listed[shuffle].astype(jnp.int32)
    first = listed[0]
    target = ((first + BEAMS // 2) % BEAMS).astype(jnp.int32)
    other = listed[target]
    listed = listed.at[0].set(other)
    listed = listed.at[target].set(first)
    return listed.astype(jnp.int32)


def draw_parents(key, part):
    return parent_table(key)


def draw_cache_keys(key, part):
    base = jax.random.normal(jax.random.fold_in(key, 7003), (BEAMS, CTX, KVH, HD), jnp.float32)
    base = jnp.clip(base, -32.0, 32.0)
    return base.reshape(BEAMS, CTX, KVH * HD).astype(jnp.bfloat16)


def draw_queries(key, part):
    base = jax.random.normal(jax.random.fold_in(key, 7004), (BEAMS, STEPS, QH, HD), jnp.float32)
    base = jnp.clip(base, -32.0, 32.0)
    return base.reshape(BEAMS, STEPS, QH * HD).astype(jnp.bfloat16)


def with_ends(result, stream_key, least, high):
    dims = result.shape
    index_at = [jax.random.randint(jax.random.fold_in(stream_key, axis), (), 0, dims[axis]) for axis in range(len(dims))]
    result = result.at[tuple(index_at)].set(least)
    longest = dims.index(max(dims))
    index_at[longest] = (index_at[longest] + 1) % dims[longest]
    return result.at[tuple(index_at)].set(high)


def shard_levels(own_key, dims, cuts, low, largest):
    def one(axis_at, blocks):
        heights = jax.random.uniform(jax.random.fold_in(jax.random.fold_in(own_key, 6), axis_at), (blocks,), jnp.float32, low / len(cuts), largest / len(cuts))
        return jnp.repeat(jnp.exp(heights), dims[axis_at] // blocks).reshape((-1,) + (1,) * (len(dims) - axis_at - 1))

    gain = one(*cuts[0])
    for cut in cuts[1:]:
        gain = gain * one(*cut)
    return gain


def noise(stream_key, dims, scale, reach, cuts=(), kind=jnp.bfloat16):
    values = scale * jax.random.normal(stream_key, dims, jnp.float32)
    if cuts:
        values = values * shard_levels(stream_key, dims, cuts, -0.22, 0.18)
    return jnp.clip(values, -reach, reach).astype(kind)


def setup_inputs(seed: int = 0, part: int = 0) -> dict:
    key_list = jax.random.split(jax.random.key(seed), 10)
    part_keys = jax.random.split(jax.random.fold_in(key_list[9], part), 10)
    cache_keys = draw_cache_keys(jax.random.fold_in(jax.random.fold_in(key_list[9], part), 71), part)
    cache_values = noise(part_keys[1], (BEAMS, CTX, KVH * HD), 1.0, 6.0, ((0, 128), (2, 2)))
    lengths = with_ends(jax.random.randint(part_keys[2], (BEAMS,), CTX // 4, CTX + 1), jax.random.fold_in(part_keys[2], 1), CTX // 4, CTX).astype(jnp.int32)
    parent_scores = jnp.clip(-6.0 + 6.0 * jax.random.uniform(part_keys[3], (BEAMS,), jnp.float32) ** shard_levels(part_keys[3], (BEAMS,), ((0, 128),), -0.2, 0.2), -6.0, 0.0)
    parents = draw_parents(jax.random.fold_in(jax.random.fold_in(key_list[9], part), 71), part)
    queries = draw_queries(jax.random.fold_in(jax.random.fold_in(key_list[9], part), 71), part)
    new_keys = noise(part_keys[6], (BEAMS, STEPS, KVH * HD), 1.5, 9.0, ((0, 128), (2, 2)))
    new_values = noise(part_keys[7], (BEAMS, STEPS, KVH * HD), 1.0, 6.0, ((0, 128), (2, 2)))
    reward_weight = noise(key_list[8], (QH * HD,), 0.5, 3.0, ((0, 2),))
    return dict(cache_keys=cache_keys, cache_values=cache_values, lengths=lengths, parent_scores=parent_scores, parents=parents, queries=queries, new_keys=new_keys, new_values=new_values, reward_weight=reward_weight)


def reference(cache_keys, cache_values, lengths, parent_scores, parents, queries, new_keys, new_values, reward_weight):
    group = QH // KVH
    scale = HD ** -0.5
    positions = jnp.arange(CTX)
    causal = jnp.arange(STEPS)[None, :] <= jnp.arange(STEPS)[:, None]

    def one_slot(index):
        parent = parents[index]
        keys = cache_keys[parent].astype(jnp.float32).reshape(CTX, KVH, HD)
        values = cache_values[parent].astype(jnp.float32).reshape(CTX, KVH, HD)
        query = queries[index].astype(jnp.float32).reshape(STEPS, KVH, group, HD)
        logits = jnp.einsum('tgjd,cgd->tgjc', query, keys) * scale
        valid = positions < lengths[parent]
        logits = jnp.where(valid[None, None, None, :], logits, -1e30)
        top_parent = jnp.max(logits, axis=-1)
        weights = jnp.exp(logits - top_parent[..., None])
        total_parent = jnp.sum(weights, axis=-1)
        rounded = weights.astype(jnp.bfloat16).astype(jnp.float32)
        sum_parent = jnp.einsum('tgjc,cgd->tgjd', rounded, values)
        parent_out = (sum_parent / total_parent[..., None]).astype(jnp.bfloat16).astype(jnp.float32)
        parent_lse = top_parent + jnp.log(total_parent)
        own_keys = new_keys[index].astype(jnp.float32).reshape(STEPS, KVH, HD)
        own_values = new_values[index].astype(jnp.float32).reshape(STEPS, KVH, HD)
        own_logits = jnp.einsum('tgjd,ugd->tgju', query, own_keys) * scale
        own_logits = jnp.where(causal[:, None, None, :], own_logits, -1e30)
        top_own = jnp.max(own_logits, axis=-1)
        own_weights = jnp.exp(own_logits - top_own[..., None])
        total_own = jnp.sum(own_weights, axis=-1)
        own_rounded = own_weights.astype(jnp.bfloat16).astype(jnp.float32)
        sum_own = jnp.einsum('tgju,ugd->tgjd', own_rounded, own_values)
        top = jnp.maximum(parent_lse, top_own)
        factor_parent = jnp.exp(parent_lse - top)
        factor_own = jnp.exp(top_own - top)
        merged = (parent_out * factor_parent[..., None] + sum_own * factor_own[..., None]) / (factor_parent + total_own * factor_own)[..., None]
        output = merged.reshape(STEPS, QH * HD).astype(jnp.bfloat16)
        reward = jnp.dot(output, reward_weight, preferred_element_type=jnp.float32)
        score = parent_scores[parent] + jnp.sum(jax.nn.log_sigmoid(reward))
        return output, score

    attended, scores = lax.map(one_slot, jnp.arange(BEAMS))
    return attended, scores
```

```python
import functools

import jax
import jax.numpy as jnp
from jax import lax
from jax.experimental import pallas as pl
from jax.experimental.pallas import tpu as pltpu
from jax.sharding import Mesh
from jax.sharding import PartitionSpec as P

HD = 128
CHILDREN = 2
META = 8
GROUPS_DP = ("groups", "z", "x")
VMEM = pl.BlockSpec(memory_space=pltpu.VMEM)
SMEM = pl.BlockSpec(memory_space=pltpu.SMEM)
BF16 = jnp.bfloat16
F32 = jnp.float32


def number_in(ref, i, row):
    return jnp.max(ref[i, row : row + META, :].astype(F32)[0:1, :]).astype(jnp.int32)


def filled(value):
    return jnp.full((META, HD), value, F32).astype(BF16)


def as_row(column):
    n = column.shape[0]
    rows = lax.broadcasted_iota(jnp.int32, (n, HD), 0)
    lanes = lax.broadcasted_iota(jnp.int32, (n, HD), 1)
    return jnp.sum(jnp.where(rows == lanes, column, 0.0), axis=0, keepdims=True)


def as_column(row):
    n = row.shape[1]
    rows = lax.broadcasted_iota(jnp.int32, (n, n), 0)
    lanes = lax.broadcasted_iota(jnp.int32, (n, n), 1)
    return jnp.sum(jnp.where(rows == lanes, row, 0.0), axis=1, keepdims=True)


def in_parts(x):
    first = x.astype(BF16)
    rest = x - first.astype(F32)
    second = rest.astype(BF16)
    third = (rest - second.astype(F32)).astype(BF16)
    return first, second, third


def items_of(q_ref, steps, heads):
    return [q_ref[0, :, h * HD : (h + 1) * HD] for h in range(heads)]


def send_kernel(parents_ref, q_ref, out_ref, item):
    steps, heads = q_ref.shape[1], q_ref.shape[2] // HD
    size = steps * heads
    for h in range(heads):
        item[h * steps : (h + 1) * steps, :] = q_ref[0, :, h * HD : (h + 1) * HD].astype(F32)
    item[size : size + META, :] = jnp.full((META, HD), parents_ref[0].astype(F32), F32)
    packed = item[...].astype(BF16)
    for d in range(out_ref.shape[0]):
        out_ref[d] = packed


def turn_kernel(columns, in_ref, out_ref, used):
    size = in_ref.shape[1] - META
    my_row, my_column = lax.axis_index("z"), lax.axis_index("x")
    for i in range(out_ref.shape[0]):
        out_ref[i, size:, :] = filled(-1.0)
    for i in range(columns):
        used[i] = 0
    for i in range(in_ref.shape[0]):
        parent = number_in(in_ref, i, size)
        row, column = parent // columns, parent % columns

        @pl.when(row == my_row)
        def _():
            place = used[column]
            used[column] = place + 1
            out_ref[column * CHILDREN + place, :size, :] = in_ref[i, :size, :]
            out_ref[column * CHILDREN + place, size:, :] = filled((i * columns + my_column).astype(F32))


def attend_kernel(kv_heads, lengths_ref, scores_ref, in_ref, k_ref, v_ref, out_ref, q, item, found):
    size = in_ref.shape[1] - META
    context = k_ref.shape[1]
    rows = size // kv_heads
    q[...] = jnp.zeros_like(q)
    found[0] = 0
    for c in range(CHILDREN):
        found[1 + c] = -1
    for i in range(in_ref.shape[0]):
        child = number_in(in_ref, i, size)

        @pl.when(child >= 0)
        def _():
            n = found[0]
            found[0] = n + 1
            found[1 + n] = child
            q[n] = in_ref[i, :size, :]

    scale = HD**-0.5
    valid = lax.broadcasted_iota(jnp.int32, (CHILDREN * rows, context), 1) < lengths_ref[0]
    totals = [[] for _ in range(CHILDREN)]
    for k in range(kv_heads):
        keys = k_ref[0, :, k * HD : (k + 1) * HD]
        values = v_ref[0, :, k * HD : (k + 1) * HD]
        both = jnp.concatenate([q[c, k * rows : (k + 1) * rows, :] for c in range(CHILDREN)], axis=0)
        logits = (
            lax.dot_general(both, keys, (((1,), (1,)), ((), ())), preferred_element_type=F32)
            * scale
        )
        logits = jnp.where(valid, logits, -1e30)
        top = jnp.max(logits, axis=-1, keepdims=True)
        weights = jnp.exp(logits - top)
        total = jnp.sum(weights, axis=-1, keepdims=True)
        summed = jnp.dot(weights.astype(BF16), values, preferred_element_type=F32)
        result = (summed / total).astype(BF16)
        log_total = top + jnp.log(total)
        for c in range(CHILDREN):
            item[c, k * rows : (k + 1) * rows, :] = result[c * rows : (c + 1) * rows, :]
            totals[c].append(log_total[c * rows : (c + 1) * rows, :])
    score = in_parts(jnp.full((1, HD), scores_ref[0], F32))
    for c in range(CHILDREN):
        line = in_parts(as_row(jnp.concatenate(totals[c], axis=0)))
        child = jnp.full((1, HD), found[1 + c].astype(F32), F32)
        tail = [child, *line, *score, jnp.zeros((1, HD), F32)]
        item[c, size:, :] = jnp.concatenate([t.astype(F32) for t in tail], axis=0).astype(BF16)
    for d in range(out_ref.shape[0] // CHILDREN):
        for c in range(CHILDREN):
            out_ref[d * CHILDREN + c] = item[c]


def back_kernel(columns, in_ref, out_ref):
    size = in_ref.shape[1] - META
    my_column = lax.axis_index("x")
    for i in range(in_ref.shape[0]):
        child = number_in(in_ref, i, size)

        @pl.when((child >= 0) & (child % columns == my_column))
        def _():
            out_ref[child // columns] = in_ref[i]


def merge_kernel(columns, parents_ref, in_ref, q_ref, nk_ref, nv_ref, rw_ref, out_ref, reward_ref, spare_ref, wide):
    size = in_ref.shape[1] - META
    steps, heads = q_ref.shape[1], q_ref.shape[2] // HD
    kv_heads = nk_ref.shape[2] // HD
    rows = size // kv_heads
    slot = parents_ref[0] // columns
    sum_parent = in_ref[slot, :size, :].astype(F32)
    tail = in_ref[slot, size:, :].astype(F32)
    top_parent = as_column((tail[1:2] + tail[2:3]) + tail[3:4])
    spare_ref[...] = jnp.broadcast_to((tail[4:5] + tail[5:6]) + tail[6:7], spare_ref.shape)
    for h in range(heads):
        wide[h * steps : (h + 1) * steps, :] = q_ref[0, :, h * HD : (h + 1) * HD].astype(F32)
    query = wide[...]
    step = lax.broadcasted_iota(jnp.int32, (size, 1), 0) % steps

    def spread(ref, u):
        return jnp.concatenate(
            [
                jnp.broadcast_to(ref[0, u : u + 1, k * HD : (k + 1) * HD].astype(F32), (rows, HD))
                for k in range(kv_heads)
            ],
            axis=0,
        )

    scale = HD**-0.5
    logits = [
        jnp.where(u <= step, jnp.sum(query * spread(nk_ref, u), axis=-1, keepdims=True) * scale, -1e30)
        for u in range(steps)
    ]
    top_own = functools.reduce(jnp.maximum, logits)
    weights = [jnp.exp(x - top_own) for x in logits]
    total_own = functools.reduce(jnp.add, weights)
    sum_own = functools.reduce(
        jnp.add, [w.astype(BF16).astype(F32) * spread(nv_ref, u) for u, w in enumerate(weights)]
    )
    top = jnp.maximum(top_parent, top_own)
    factor_parent = jnp.exp(top_parent - top)
    factor_own = jnp.exp(top_own - top)
    merged = (sum_parent * factor_parent + sum_own * factor_own) / (
        factor_parent + total_own * factor_own
    )
    attended = merged.astype(BF16).astype(F32)
    wide[...] = attended
    reward = jnp.zeros((steps, HD), F32)
    for h in range(heads):
        part = wide[h * steps : (h + 1) * steps, :]
        out_ref[0, :, h * HD : (h + 1) * HD] = part.astype(BF16)
        reward = reward + part * rw_ref[0:1, h * HD : (h + 1) * HD].astype(F32)
    reward_ref[...] = jnp.broadcast_to(jnp.sum(reward, axis=-1, keepdims=True), reward_ref.shape)


def per_device(
    cache_keys,
    cache_values,
    lengths,
    parent_scores,
    parents,
    queries,
    new_keys,
    new_values,
    reward_weight,
):
    z, x = lax.axis_size("z"), lax.axis_size("x")
    steps, width = queries.shape[1:]
    heads = width // HD
    kv_heads = cache_keys.shape[2] // HD
    size = steps * heads
    tall = size + META

    def items(n):
        return jax.ShapeDtypeStruct((n, tall, HD), BF16)

    sent = pl.pallas_call(
        send_kernel,
        out_shape=items(z),
        in_specs=[SMEM, VMEM],
        out_specs=VMEM,
        scratch_shapes=[pltpu.VMEM((tall, HD), F32)],
        name="send",
    )(parents, queries)
    column = lax.all_to_all(sent, "z", 0, 0, tiled=True)
    turned = pl.pallas_call(
        functools.partial(turn_kernel, x),
        out_shape=items(x * CHILDREN),
        in_specs=[VMEM],
        out_specs=VMEM,
        scratch_shapes=[pltpu.SMEM((x,), jnp.int32)],
        name="turn",
    )(column)
    row = lax.all_to_all(turned, "x", 0, 0, tiled=True)
    outputs = pl.pallas_call(
        functools.partial(attend_kernel, kv_heads),
        out_shape=items(x * CHILDREN),
        in_specs=[SMEM, SMEM, VMEM, VMEM, VMEM],
        out_specs=VMEM,
        scratch_shapes=[
            pltpu.VMEM((CHILDREN, size, HD), BF16),
            pltpu.VMEM((CHILDREN, tall, HD), BF16),
            pltpu.SMEM((1 + CHILDREN,), jnp.int32),
        ],
        name="attend",
    )(lengths, parent_scores, row, cache_keys, cache_values)
    row = lax.all_to_all(outputs, "x", 0, 0, tiled=True)
    back = pl.pallas_call(
        functools.partial(back_kernel, x),
        out_shape=items(z),
        in_specs=[VMEM],
        out_specs=VMEM,
        name="back",
    )(row)
    column = lax.all_to_all(back, "z", 0, 0, tiled=True)
    output, partial_reward, inherited = pl.pallas_call(
        functools.partial(merge_kernel, x),
        out_shape=(
            jax.ShapeDtypeStruct(queries.shape, BF16),
            jax.ShapeDtypeStruct((steps, HD), F32),
            jax.ShapeDtypeStruct((1, HD), F32),
        ),
        in_specs=[SMEM, VMEM, VMEM, VMEM, VMEM, VMEM],
        out_specs=(VMEM, VMEM, VMEM),
        scratch_shapes=[pltpu.VMEM((size, HD), F32)],
        name="merge",
    )(parents, column, queries, new_keys, new_values, reward_weight.reshape(1, width))
    reward = lax.psum(partial_reward, "tensor")[:, 0]
    score = inherited[0, :1] + jnp.sum(jax.nn.log_sigmoid(reward))
    return (output, score)


def solution(mesh):
    finer = Mesh(
        mesh.devices.reshape(mesh.shape["groups"], 16, 8, mesh.shape["tensor"]),
        ("groups", "z", "x", "tensor"),
    )
    return jax.shard_map(
        per_device,
        mesh=finer,
        in_specs=(
            P(GROUPS_DP, None, "tensor"),
            P(GROUPS_DP, None, "tensor"),
            P(GROUPS_DP),
            P(GROUPS_DP),
            P(GROUPS_DP),
            P(GROUPS_DP, None, "tensor"),
            P(GROUPS_DP, None, "tensor"),
            P(GROUPS_DP, None, "tensor"),
            P("tensor"),
        ),
        out_specs=(P(GROUPS_DP, None, "tensor"), P(GROUPS_DP)),
        check_vma=False,
    )
```

```python
import functools

import jax
import jax.numpy as jnp
from jax import lax
from jax.experimental import pallas as pl
from jax.experimental.pallas import tpu as pltpu
from jax.sharding import Mesh
from jax.sharding import PartitionSpec as P

HD = 128
CHILDREN = 2
META = 8
GROUPS_DP = ("groups", "zh", "zl", "x")
NEAR = ("zl", "x")
FAR = ("zh", "zl")
VMEM = pl.BlockSpec(memory_space=pltpu.VMEM)
SMEM = pl.BlockSpec(memory_space=pltpu.SMEM)
BF16 = jnp.bfloat16
F32 = jnp.float32


def limit(mib):
    return pltpu.CompilerParams(vmem_limit_bytes=mib * 1024 * 1024)


def whole_number(row, lane):
    return jnp.sum(row[:, lane : lane + 1]).astype(jnp.int32)


def in_parts(x):
    first = x.astype(BF16)
    rest = x - first.astype(F32)
    second = rest.astype(BF16)
    third = (rest - second.astype(F32)).astype(BF16)
    return [part.astype(F32) for part in (first, second, third)]


def send_kernel(columns, parents_ref, q_ref, out_ref, item):
    steps, heads = q_ref.shape[1], q_ref.shape[2] // HD
    rows = out_ref.shape[1] - META
    for h in range(heads):
        item[h * steps : (h + 1) * steps, :] = q_ref[0, :, h * HD : (h + 1) * HD].astype(F32)
    parent = jnp.full((META, HD), parents_ref[0].astype(F32), F32).astype(BF16)
    for j in range(out_ref.shape[0] // columns):
        piece = item[j * rows : (j + 1) * rows, :].astype(BF16)
        for d in range(columns):
            out_ref[j * columns + d, :rows, :] = piece
            out_ref[j * columns + d, rows:, :] = parent


def turn_kernel(columns, in_ref, out_ref, used, meta):
    rows = in_ref.shape[1] - META
    block = in_ref.shape[0] // columns
    first = lax.axis_index("zh") * block
    mine = lax.axis_index("x")
    parents = [whole_number(in_ref[i, rows:, :].astype(F32)[0:1], 0) for i in range(in_ref.shape[0])]
    meta[...] = jnp.full(meta.shape, -1.0, F32)
    for i in range(out_ref.shape[0]):
        used[i] = 0
    for i, parent in enumerate(parents):

        @pl.when(parent % columns == mine)
        def _():
            row = parent // columns
            place = used[row]
            used[row] = place + 1
            out_ref[row, pl.ds(pl.multiple_of(place * rows, rows), rows), :] = in_ref[i, :rows, :]
            child = first * columns + i
            meta[row, pl.ds(place, 1), :] = jnp.full((1, HD), child.astype(F32), F32)

    for i in range(out_ref.shape[0]):
        out_ref[i, CHILDREN * rows :, :] = meta[i].astype(BF16)


def attend_kernel(lengths_ref, scores_ref, in_ref, k_ref, v_ref, out_ref, q, item, found):
    kv_heads, tall = item.shape[:2]
    rows = (tall - META) // CHILDREN
    context = k_ref.shape[1]
    blocks = in_ref.shape[0] // kv_heads
    ids = []
    for b in range(blocks):
        tail = in_ref[b * kv_heads, CHILDREN * rows :, :].astype(F32)
        ids.append([whole_number(tail[c : c + 1], 0) for c in range(CHILDREN)])
    q[...] = jnp.zeros_like(q)
    found[0] = 0
    for c in range(CHILDREN):
        found[1 + c] = -1
    for b in range(blocks):
        for c in range(CHILDREN):

            @pl.when(ids[b][c] >= 0)
            def _():
                n = found[0]
                found[0] = n + 1
                found[1 + n] = ids[b][c]
                for j in range(kv_heads):
                    piece = in_ref[b * kv_heads + j, c * rows : (c + 1) * rows, :]
                    q[j, pl.ds(pl.multiple_of(n * rows, rows), rows), :] = piece

    scale = HD**-0.5
    valid = lax.broadcasted_iota(jnp.int32, (CHILDREN * rows, context), 1) < lengths_ref[0]
    lane = lax.broadcasted_iota(jnp.int32, (rows, HD), 1)
    diagonal = lane % rows == lax.broadcasted_iota(jnp.int32, (rows, HD), 0)
    part = lax.broadcasted_iota(jnp.int32, (1, HD), 1)
    score = in_parts(jnp.full((1, HD), scores_ref[0], F32))
    for j in range(kv_heads):
        keys = k_ref[0, :, j * HD : (j + 1) * HD]
        values = v_ref[0, :, j * HD : (j + 1) * HD]
        logits = (
            lax.dot_general(q[j], keys, (((1,), (1,)), ((), ())), preferred_element_type=F32)
            * scale
        )
        logits = jnp.where(valid, logits, -1e30)
        top = jnp.max(logits, axis=-1, keepdims=True)
        weights = jnp.exp(logits - top)
        total = jnp.sum(weights, axis=-1, keepdims=True)
        summed = jnp.dot(weights.astype(BF16), values, preferred_element_type=F32)
        item[j, : CHILDREN * rows, :] = (summed / total).astype(BF16)
        log_total = top + jnp.log(total)
        tails = []
        for c in range(CHILDREN):
            parts = in_parts(jnp.broadcast_to(log_total[c * rows : (c + 1) * rows], (rows, HD)))
            chosen = jnp.where(
                lane < rows, parts[0], jnp.where(lane < 2 * rows, parts[1], parts[2])
            )
            line = jnp.sum(jnp.where(diagonal, chosen, 0.0), axis=0, keepdims=True)
            for n, extra in enumerate([jnp.full((1, HD), found[1 + c].astype(F32), F32), *score]):
                line = jnp.where(part == 3 * rows + n, extra, line)
            tails.append(line)
        tails.append(jnp.zeros((META - CHILDREN, HD), F32))
        item[j, CHILDREN * rows :, :] = jnp.concatenate(tails, axis=0).astype(BF16)
    for b in range(blocks):
        out_ref[b * kv_heads : (b + 1) * kv_heads] = item[...]


def back_kernel(columns, in_ref, out_ref):
    rows = out_ref.shape[1] - META
    first = lax.axis_index("zh") * out_ref.shape[0]
    children = []
    for i in range(in_ref.shape[0]):
        tail = in_ref[i, CHILDREN * rows :, :].astype(F32)
        children.append([whole_number(tail[c : c + 1], 3 * rows) for c in range(CHILDREN)])
    for i in range(in_ref.shape[0]):
        for c in range(CHILDREN):
            place = children[i][c] - first

            @pl.when((place >= 0) & (place < out_ref.shape[0]))
            def _():
                out_ref[place, :rows, :] = in_ref[i, c * rows : (c + 1) * rows, :]
                tail = in_ref[i, CHILDREN * rows :, :].astype(F32)[c : c + 1]
                out_ref[place, rows:, :] = jnp.broadcast_to(tail, (META, HD)).astype(BF16)


def merge_kernel(
    columns, parents_ref, in_ref, q_ref, nk_ref, nv_ref, rw_ref, out_ref, reward_ref, spare_ref, wide
):
    rows = in_ref.shape[1] - META
    steps, heads = q_ref.shape[1], q_ref.shape[2] // HD
    kv_heads = nk_ref.shape[2] // HD
    size = steps * heads
    column = parents_ref[0] % columns
    lane = lax.broadcasted_iota(jnp.int32, (rows, HD), 1)
    own = lane % rows == lax.broadcasted_iota(jnp.int32, (rows, HD), 0)
    own = own & (lane < 3 * rows)
    sums, tops = [], []
    for j in range(kv_heads):
        sums.append(in_ref[j * columns + column, :rows, :].astype(F32))
        tail = in_ref[j * columns + column, rows:, :].astype(F32)[0:1]
        tops.append(jnp.sum(jnp.where(own, tail, 0.0), axis=-1, keepdims=True))
        if j == 0:
            base = 3 * rows + 1
            inherited = (tail[:, base : base + 1] + tail[:, base + 1 : base + 2]) + tail[:, base + 2 : base + 3]
            spare_ref[...] = jnp.broadcast_to(inherited, spare_ref.shape)
    sum_parent = jnp.concatenate(sums, axis=0)
    top_parent = jnp.concatenate(tops, axis=0)
    for h in range(heads):
        wide[h * steps : (h + 1) * steps, :] = q_ref[0, :, h * HD : (h + 1) * HD].astype(F32)
    query = wide[...]
    step = lax.broadcasted_iota(jnp.int32, (size, 1), 0) % steps

    def spread(ref, u):
        return jnp.concatenate(
            [
                jnp.broadcast_to(ref[0, u : u + 1, k * HD : (k + 1) * HD].astype(F32), (rows, HD))
                for k in range(kv_heads)
            ],
            axis=0,
        )

    scale = HD**-0.5
    logits = [
        jnp.where(u <= step, jnp.sum(query * spread(nk_ref, u), axis=-1, keepdims=True) * scale, -1e30)
        for u in range(steps)
    ]
    top_own = functools.reduce(jnp.maximum, logits)
    weights = [jnp.exp(x - top_own) for x in logits]
    total_own = functools.reduce(jnp.add, weights)
    sum_own = functools.reduce(
        jnp.add, [w.astype(BF16).astype(F32) * spread(nv_ref, u) for u, w in enumerate(weights)]
    )
    top = jnp.maximum(top_parent, top_own)
    factor_parent = jnp.exp(top_parent - top)
    factor_own = jnp.exp(top_own - top)
    merged = (sum_parent * factor_parent + sum_own * factor_own) / (
        factor_parent + total_own * factor_own
    )
    attended = merged.astype(BF16).astype(F32)
    wide[...] = attended
    reward = jnp.zeros((steps, HD), F32)
    for h in range(heads):
        part = wide[h * steps : (h + 1) * steps, :]
        out_ref[0, :, h * HD : (h + 1) * HD] = part.astype(BF16)
        reward = reward + part * rw_ref[0:1, h * HD : (h + 1) * HD].astype(F32)
    reward_ref[...] = jnp.broadcast_to(jnp.sum(reward, axis=-1, keepdims=True), reward_ref.shape)


def per_device(
    cache_keys,
    cache_values,
    lengths,
    parent_scores,
    parents,
    queries,
    new_keys,
    new_values,
    reward_weight,
):
    columns = lax.axis_size("x")
    near, far = lax.axis_size(NEAR), lax.axis_size(FAR)
    steps, width = queries.shape[1:]
    heads = width // HD
    kv_heads = cache_keys.shape[2] // HD
    size = steps * heads
    rows = size // kv_heads
    tall = CHILDREN * rows + META

    def array(*shape, kind=BF16):
        return jax.ShapeDtypeStruct(shape, kind)

    sent = pl.pallas_call(
        functools.partial(send_kernel, columns),
        out_shape=array(near, rows + META, HD),
        in_specs=[SMEM, VMEM],
        out_specs=VMEM,
        scratch_shapes=[pltpu.VMEM((size, HD), F32)],
        compiler_params=limit(4),
        name="send",
    )(parents, queries)
    pieces = lax.all_to_all(sent, NEAR, 0, 0, tiled=True)
    turned = pl.pallas_call(
        functools.partial(turn_kernel, columns),
        out_shape=array(far, tall, HD),
        in_specs=[VMEM],
        out_specs=VMEM,
        scratch_shapes=[pltpu.SMEM((far,), jnp.int32), pltpu.VMEM((far, META, HD), F32)],
        compiler_params=limit(4),
        name="turn",
    )(pieces)
    asked = lax.all_to_all(turned, FAR, 0, 0, tiled=True)
    outputs = pl.pallas_call(
        attend_kernel,
        out_shape=array(far, tall, HD),
        in_specs=[SMEM, SMEM, VMEM, VMEM, VMEM],
        out_specs=VMEM,
        scratch_shapes=[
            pltpu.VMEM((kv_heads, CHILDREN * rows, HD), BF16),
            pltpu.VMEM((kv_heads, tall, HD), BF16),
            pltpu.SMEM((1 + CHILDREN,), jnp.int32),
        ],
        compiler_params=limit(16),
        name="attend",
    )(lengths, parent_scores, asked, cache_keys, cache_values)
    answers = lax.all_to_all(outputs, FAR, 0, 0, tiled=True)
    back = pl.pallas_call(
        functools.partial(back_kernel, columns),
        out_shape=array(near, rows + META, HD),
        in_specs=[VMEM],
        out_specs=VMEM,
        compiler_params=limit(4),
        name="back",
    )(answers)
    pieces = lax.all_to_all(back, NEAR, 0, 0, tiled=True)
    output, partial_reward, inherited = pl.pallas_call(
        functools.partial(merge_kernel, columns),
        out_shape=(
            array(*queries.shape),
            array(steps, HD, kind=F32),
            array(1, HD, kind=F32),
        ),
        in_specs=[SMEM, VMEM, VMEM, VMEM, VMEM, VMEM],
        out_specs=(VMEM, VMEM, VMEM),
        scratch_shapes=[pltpu.VMEM((size, HD), F32)],
        compiler_params=limit(4),
        name="merge",
    )(parents, pieces, queries, new_keys, new_values, reward_weight.reshape(1, width))
    reward = lax.psum(partial_reward, "tensor")[:, 0]
    score = inherited[0, :1] + jnp.sum(jax.nn.log_sigmoid(reward))
    return (output, score)


def solution(mesh):
    finer = Mesh(
        mesh.devices.reshape(mesh.shape["groups"], 4, 4, 8, mesh.shape["tensor"]),
        ("groups", "zh", "zl", "x", "tensor"),
    )
    return jax.shard_map(
        per_device,
        mesh=finer,
        in_specs=(
            P(GROUPS_DP, None, "tensor"),
            P(GROUPS_DP, None, "tensor"),
            P(GROUPS_DP),
            P(GROUPS_DP),
            P(GROUPS_DP),
            P(GROUPS_DP, None, "tensor"),
            P(GROUPS_DP, None, "tensor"),
            P(GROUPS_DP, None, "tensor"),
            P("tensor"),
        ),
        out_specs=(P(GROUPS_DP, None, "tensor"), P(GROUPS_DP)),
        check_vma=False,
    )
```

```python
import functools

import jax
import jax.numpy as jnp
from jax import lax
from jax.experimental import pallas as pl
from jax.experimental.pallas import tpu as pltpu
from jax.sharding import Mesh
from jax.sharding import PartitionSpec as P

HD = 128
CHILDREN = 2
META = 8
GROUPS_DP = ("groups", "zh", "zl", "x")
NEAR = ("zl", "x")
FAR = ("zh", "zl")
VMEM = pl.BlockSpec(memory_space=pltpu.VMEM)
SMEM = pl.BlockSpec(memory_space=pltpu.SMEM)
BF16 = jnp.bfloat16
F32 = jnp.float32
SLOW = pl.CostEstimate(flops=10**10, bytes_accessed=2**26, transcendentals=0)


def limit(mib):
    return pltpu.CompilerParams(vmem_limit_bytes=mib * 1024 * 1024)


def whole_number(row, lane):
    return jnp.sum(row[:, lane : lane + 1]).astype(jnp.int32)


def in_parts(x):
    first = x.astype(BF16)
    rest = x - first.astype(F32)
    second = rest.astype(BF16)
    third = (rest - second.astype(F32)).astype(BF16)
    return [part.astype(F32) for part in (first, second, third)]


def send_kernel(columns, parents_ref, lengths_ref, scores_ref, q_ref, out_ref, item):
    steps, heads = q_ref.shape[1], q_ref.shape[2] // HD
    rows = out_ref.shape[1] - META
    for h in range(heads):
        item[h * steps : (h + 1) * steps, :] = q_ref[0, :, h * HD : (h + 1) * HD].astype(F32)
    parent = jnp.full((META, HD), parents_ref[0].astype(F32), F32).astype(BF16)
    for j in range(out_ref.shape[0] // columns):
        piece = item[j * rows : (j + 1) * rows, :].astype(BF16)
        for d in range(columns):
            out_ref[j * columns + d, :rows, :] = piece
            out_ref[j * columns + d, rows:, :] = parent


def turn_kernel(columns, in_ref, out_ref, used, meta):
    rows = in_ref.shape[1] - META
    block = in_ref.shape[0] // columns
    first = lax.axis_index("zh") * block
    mine = lax.axis_index("x")
    parents = [whole_number(in_ref[i, rows:, :].astype(F32)[0:1], 0) for i in range(in_ref.shape[0])]
    meta[...] = jnp.full(meta.shape, -1.0, F32)
    for i in range(out_ref.shape[0]):
        used[i] = 0
    for i, parent in enumerate(parents):

        @pl.when(parent % columns == mine)
        def _():
            row = parent // columns
            place = used[row]
            used[row] = place + 1
            out_ref[row, pl.ds(pl.multiple_of(place * rows, rows), rows), :] = in_ref[i, :rows, :]
            child = first * columns + i
            meta[row, pl.ds(place, 1), :] = jnp.full((1, HD), child.astype(F32), F32)

    for i in range(out_ref.shape[0]):
        out_ref[i, CHILDREN * rows :, :] = meta[i].astype(BF16)


def attend_kernel(lengths_ref, scores_ref, in_ref, k_ref, v_ref, out_ref, q, item, found):
    kv_heads, tall = item.shape[:2]
    rows = (tall - META) // CHILDREN
    context = k_ref.shape[1]
    blocks = in_ref.shape[0] // kv_heads
    ids = []
    for b in range(blocks):
        tail = in_ref[b * kv_heads, CHILDREN * rows :, :].astype(F32)
        ids.append([whole_number(tail[c : c + 1], 0) for c in range(CHILDREN)])
    q[...] = jnp.zeros_like(q)
    found[0] = 0
    for c in range(CHILDREN):
        found[1 + c] = -1
    for b in range(blocks):
        for c in range(CHILDREN):

            @pl.when(ids[b][c] >= 0)
            def _():
                n = found[0]
                found[0] = n + 1
                found[1 + n] = ids[b][c]
                for j in range(kv_heads):
                    piece = in_ref[b * kv_heads + j, c * rows : (c + 1) * rows, :]
                    q[j, pl.ds(pl.multiple_of(n * rows, rows), rows), :] = piece

    scale = HD**-0.5
    valid = lax.broadcasted_iota(jnp.int32, (CHILDREN * rows, context), 1) < lengths_ref[0]
    lane = lax.broadcasted_iota(jnp.int32, (rows, HD), 1)
    diagonal = lane % rows == lax.broadcasted_iota(jnp.int32, (rows, HD), 0)
    part = lax.broadcasted_iota(jnp.int32, (1, HD), 1)
    score = in_parts(jnp.full((1, HD), scores_ref[0], F32))
    for j in range(kv_heads):
        keys = k_ref[0, :, j * HD : (j + 1) * HD]
        values = v_ref[0, :, j * HD : (j + 1) * HD]
        logits = (
            lax.dot_general(q[j], keys, (((1,), (1,)), ((), ())), preferred_element_type=F32)
            * scale
        )
        logits = jnp.where(valid, logits, -1e30)
        top = jnp.max(logits, axis=-1, keepdims=True)
        weights = jnp.exp(logits - top)
        total = jnp.sum(weights, axis=-1, keepdims=True)
        summed = jnp.dot(weights.astype(BF16), values, preferred_element_type=F32)
        item[j, : CHILDREN * rows, :] = (summed / total).astype(BF16)
        log_total = top + jnp.log(total)
        tails = []
        for c in range(CHILDREN):
            parts = in_parts(jnp.broadcast_to(log_total[c * rows : (c + 1) * rows], (rows, HD)))
            chosen = jnp.where(
                lane < rows, parts[0], jnp.where(lane < 2 * rows, parts[1], parts[2])
            )
            line = jnp.sum(jnp.where(diagonal, chosen, 0.0), axis=0, keepdims=True)
            for n, extra in enumerate([jnp.full((1, HD), found[1 + c].astype(F32), F32), *score]):
                line = jnp.where(part == 3 * rows + n, extra, line)
            tails.append(line)
        tails.append(jnp.zeros((META - CHILDREN, HD), F32))
        item[j, CHILDREN * rows :, :] = jnp.concatenate(tails, axis=0).astype(BF16)
    for b in range(blocks):
        out_ref[b * kv_heads : (b + 1) * kv_heads] = item[...]


def back_kernel(columns, in_ref, out_ref):
    rows = out_ref.shape[1] - META
    first = lax.axis_index("zh") * out_ref.shape[0]
    children = []
    for i in range(in_ref.shape[0]):
        tail = in_ref[i, CHILDREN * rows :, :].astype(F32)
        children.append([whole_number(tail[c : c + 1], 3 * rows) for c in range(CHILDREN)])
    for i in range(in_ref.shape[0]):
        for c in range(CHILDREN):
            place = children[i][c] - first

            @pl.when((place >= 0) & (place < out_ref.shape[0]))
            def _():
                out_ref[place, :rows, :] = in_ref[i, c * rows : (c + 1) * rows, :]
                tail = in_ref[i, CHILDREN * rows :, :].astype(F32)[c : c + 1]
                out_ref[place, rows:, :] = jnp.broadcast_to(tail, (META, HD)).astype(BF16)


def merge_kernel(
    columns, parents_ref, in_ref, q_ref, nk_ref, nv_ref, rw_ref, out_ref, reward_ref, spare_ref, wide
):
    rows = in_ref.shape[1] - META
    steps, heads = q_ref.shape[1], q_ref.shape[2] // HD
    kv_heads = nk_ref.shape[2] // HD
    size = steps * heads
    column = parents_ref[0] % columns
    lane = lax.broadcasted_iota(jnp.int32, (rows, HD), 1)
    own = lane % rows == lax.broadcasted_iota(jnp.int32, (rows, HD), 0)
    own = own & (lane < 3 * rows)
    sums, tops = [], []
    for j in range(kv_heads):
        sums.append(in_ref[j * columns + column, :rows, :].astype(F32))
        tail = in_ref[j * columns + column, rows:, :].astype(F32)[0:1]
        tops.append(jnp.sum(jnp.where(own, tail, 0.0), axis=-1, keepdims=True))
        if j == 0:
            base = 3 * rows + 1
            inherited = (tail[:, base : base + 1] + tail[:, base + 1 : base + 2]) + tail[:, base + 2 : base + 3]
            spare_ref[...] = jnp.broadcast_to(inherited, spare_ref.shape)
    sum_parent = jnp.concatenate(sums, axis=0)
    top_parent = jnp.concatenate(tops, axis=0)
    for h in range(heads):
        wide[h * steps : (h + 1) * steps, :] = q_ref[0, :, h * HD : (h + 1) * HD].astype(F32)
    query = wide[...]
    step = lax.broadcasted_iota(jnp.int32, (size, 1), 0) % steps

    def spread(ref, u):
        return jnp.concatenate(
            [
                jnp.broadcast_to(ref[0, u : u + 1, k * HD : (k + 1) * HD].astype(F32), (rows, HD))
                for k in range(kv_heads)
            ],
            axis=0,
        )

    scale = HD**-0.5
    logits = [
        jnp.where(u <= step, jnp.sum(query * spread(nk_ref, u), axis=-1, keepdims=True) * scale, -1e30)
        for u in range(steps)
    ]
    top_own = functools.reduce(jnp.maximum, logits)
    weights = [jnp.exp(x - top_own) for x in logits]
    total_own = functools.reduce(jnp.add, weights)
    sum_own = functools.reduce(
        jnp.add, [w.astype(BF16).astype(F32) * spread(nv_ref, u) for u, w in enumerate(weights)]
    )
    top = jnp.maximum(top_parent, top_own)
    factor_parent = jnp.exp(top_parent - top)
    factor_own = jnp.exp(top_own - top)
    merged = (sum_parent * factor_parent + sum_own * factor_own) / (
        factor_parent + total_own * factor_own
    )
    attended = merged.astype(BF16).astype(F32)
    wide[...] = attended
    reward = jnp.zeros((steps, HD), F32)
    for h in range(heads):
        part = wide[h * steps : (h + 1) * steps, :]
        out_ref[0, :, h * HD : (h + 1) * HD] = part.astype(BF16)
        reward = reward + part * rw_ref[h * HD : (h + 1) * HD].astype(F32)[None, :]
    reward_ref[...] = jnp.broadcast_to(jnp.sum(reward, axis=-1, keepdims=True), reward_ref.shape)


def per_device(
    cache_keys,
    cache_values,
    lengths,
    parent_scores,
    parents,
    queries,
    new_keys,
    new_values,
    reward_weight,
):
    columns = lax.axis_size("x")
    near, far = lax.axis_size(NEAR), lax.axis_size(FAR)
    steps, width = queries.shape[1:]
    heads = width // HD
    kv_heads = cache_keys.shape[2] // HD
    size = steps * heads
    rows = size // kv_heads
    tall = CHILDREN * rows + META

    def array(*shape, kind=BF16):
        return jax.ShapeDtypeStruct(shape, kind)

    sent = pl.pallas_call(
        functools.partial(send_kernel, columns),
        out_shape=array(near, rows + META, HD),
        in_specs=[SMEM, SMEM, SMEM, VMEM],
        out_specs=VMEM,
        scratch_shapes=[pltpu.VMEM((size, HD), F32)],
        compiler_params=limit(4),
        cost_estimate=SLOW,
        name="send",
    )(parents, lengths, parent_scores, queries)
    pieces = lax.all_to_all(sent, NEAR, 0, 0, tiled=True)
    turned = pl.pallas_call(
        functools.partial(turn_kernel, columns),
        out_shape=array(far, tall, HD),
        in_specs=[VMEM],
        out_specs=VMEM,
        scratch_shapes=[pltpu.SMEM((far,), jnp.int32), pltpu.VMEM((far, META, HD), F32)],
        compiler_params=limit(4),
        cost_estimate=SLOW,
        name="turn",
    )(pieces)
    asked = lax.all_to_all(turned, FAR, 0, 0, tiled=True)
    outputs = pl.pallas_call(
        attend_kernel,
        out_shape=array(far, tall, HD),
        in_specs=[SMEM, SMEM, VMEM, VMEM, VMEM],
        out_specs=VMEM,
        scratch_shapes=[
            pltpu.VMEM((kv_heads, CHILDREN * rows, HD), BF16),
            pltpu.VMEM((kv_heads, tall, HD), BF16),
            pltpu.SMEM((1 + CHILDREN,), jnp.int32),
        ],
        compiler_params=limit(16),
        name="attend",
    )(lengths, parent_scores, asked, cache_keys, cache_values)
    answers = lax.all_to_all(outputs, FAR, 0, 0, tiled=True)
    back = pl.pallas_call(
        functools.partial(back_kernel, columns),
        out_shape=array(near, rows + META, HD),
        in_specs=[VMEM],
        out_specs=VMEM,
        compiler_params=limit(4),
        name="back",
    )(answers)
    pieces = lax.all_to_all(back, NEAR, 0, 0, tiled=True)
    output, partial_reward, inherited = pl.pallas_call(
        functools.partial(merge_kernel, columns),
        out_shape=(
            array(*queries.shape),
            array(steps, HD, kind=F32),
            array(1, HD, kind=F32),
        ),
        in_specs=[SMEM, VMEM, VMEM, VMEM, VMEM, VMEM],
        out_specs=(VMEM, VMEM, VMEM),
        scratch_shapes=[pltpu.VMEM((size, HD), F32)],
        compiler_params=limit(4),
        name="merge",
    )(parents, pieces, queries, new_keys, new_values, reward_weight)
    reward = lax.psum(partial_reward, "tensor")[:, 0]
    score = inherited[0, :1] + jnp.sum(jax.nn.log_sigmoid(reward))
    return (output, score)


def solution(mesh):
    finer = Mesh(
        mesh.devices.reshape(mesh.shape["groups"], 4, 4, 8, mesh.shape["tensor"]),
        ("groups", "zh", "zl", "x", "tensor"),
    )
    return jax.shard_map(
        per_device,
        mesh=finer,
        in_specs=(
            P(GROUPS_DP, None, "tensor"),
            P(GROUPS_DP, None, "tensor"),
            P(GROUPS_DP),
            P(GROUPS_DP),
            P(GROUPS_DP),
            P(GROUPS_DP, None, "tensor"),
            P(GROUPS_DP, None, "tensor"),
            P(GROUPS_DP, None, "tensor"),
            P("tensor"),
        ),
        out_specs=(P(GROUPS_DP, None, "tensor"), P(GROUPS_DP)),
        check_vma=False,
    )
```

```python
import functools

import jax
import jax.numpy as jnp
from jax import lax
from jax.experimental import pallas as pl
from jax.experimental.pallas import tpu as pltpu
from jax.sharding import Mesh
from jax.sharding import PartitionSpec as P

HD = 128
CHILDREN = 2
PAIR = 2
TILE = 8
GROUPS_DP = ("groups", "zh", "zl", "x")
NEAR = ("zl", "x")
FAR = ("zh", "zl")
VMEM = pl.BlockSpec(memory_space=pltpu.VMEM)
SMEM = pl.BlockSpec(memory_space=pltpu.SMEM)
BF16 = jnp.bfloat16
F32 = jnp.float32
SLOW = pl.CostEstimate(flops=10**10, bytes_accessed=2**26, transcendentals=0)


def limit(mib):
    return pltpu.CompilerParams(vmem_limit_bytes=mib * 1024 * 1024)


def whole_number(row, lane):
    return jnp.sum(row[:, lane : lane + 1]).astype(jnp.int32)


def in_parts(x):
    first = x.astype(BF16)
    rest = x - first.astype(F32)
    second = rest.astype(BF16)
    third = (rest - second.astype(F32)).astype(BF16)
    return [part.astype(F32) for part in (first, second, third)]


def send_kernel(columns, parents_ref, lengths_ref, scores_ref, q_ref, out_ref, facts_ref):
    steps = q_ref.shape[1]
    pairs = out_ref.shape[1] - 1
    turns = steps // PAIR
    facts = [parents_ref[0].astype(F32), lengths_ref[0].astype(F32), scores_ref[0]]
    for n, fact in enumerate(facts):
        facts_ref[n : n + 1, :] = jnp.full((1, HD), fact, F32)
    parent = jnp.full((PAIR, HD), facts[0], F32).astype(BF16)
    for j in range(out_ref.shape[0] // columns):
        for g in range(pairs):
            h, t = j * (pairs // turns) + g // turns, g % turns * PAIR
            pair = q_ref[0, t : t + PAIR, h * HD : (h + 1) * HD]
            for d in range(columns):
                out_ref[j * columns + d, g] = pair
        for d in range(columns):
            out_ref[j * columns + d, pairs] = parent


def turn_kernel(columns, in_ref, out_ref, used, meta):
    pairs = in_ref.shape[1] - 1
    block = in_ref.shape[0] // columns
    first = lax.axis_index("zh") * block
    mine = lax.axis_index("x")
    parents = [whole_number(in_ref[i, pairs].astype(F32)[0:1], 0) for i in range(in_ref.shape[0])]
    meta[...] = jnp.full(meta.shape, -1.0, F32)
    for i in range(out_ref.shape[0]):
        used[i] = 0
    for i, parent in enumerate(parents):

        @pl.when(parent % columns == mine)
        def _():
            row = parent // columns
            place = used[row]
            used[row] = place + 1
            out_ref[row, pl.ds(place * pairs, pairs)] = in_ref[i, :pairs]
            child = first * columns + i
            meta[row, pl.ds(place, 1), :] = jnp.full((1, HD), child.astype(F32), F32)

    for i in range(out_ref.shape[0]):
        out_ref[i, CHILDREN * pairs] = meta[i, :CHILDREN, :].astype(BF16)


def attend_kernel(facts_ref, in_ref, k_ref, v_ref, out_ref, q, result, item, found):
    kv_heads = item.shape[0]
    pairs = in_ref.shape[1] // CHILDREN
    rows = pairs * PAIR
    context = k_ref.shape[1]
    blocks = in_ref.shape[0] // kv_heads
    ids = []
    for b in range(blocks):
        tail = in_ref[b * kv_heads, CHILDREN * pairs].astype(F32)
        ids.append([whole_number(tail[c : c + 1], 0) for c in range(CHILDREN)])
    q[...] = jnp.zeros_like(q)
    found[0] = 0
    for c in range(CHILDREN):
        found[1 + c] = -1
    for b in range(blocks):
        for c in range(CHILDREN):

            @pl.when(ids[b][c] >= 0)
            def _():
                n = found[0]
                found[0] = n + 1
                found[1 + n] = ids[b][c]
                for j in range(kv_heads):
                    for g in range(pairs):
                        pair = in_ref[b * kv_heads + j, c * pairs + g].astype(F32)
                        q[j, n, g * PAIR : (g + 1) * PAIR, :] = pair

    scale = HD**-0.5
    length = facts_ref[1:2, 0:1].astype(jnp.int32)
    valid = lax.broadcasted_iota(jnp.int32, (CHILDREN * rows, context), 1) < length
    lane = lax.broadcasted_iota(jnp.int32, (rows, HD), 1)
    diagonal = lane % rows == lax.broadcasted_iota(jnp.int32, (rows, HD), 0)
    part = lax.broadcasted_iota(jnp.int32, (1, HD), 1)
    score = in_parts(facts_ref[2:3, :])
    for j in range(kv_heads):
        keys = k_ref[0, :, j * HD : (j + 1) * HD]
        values = v_ref[0, :, j * HD : (j + 1) * HD]
        query = q[j].reshape(CHILDREN * rows, HD).astype(BF16)
        logits = (
            lax.dot_general(query, keys, (((1,), (1,)), ((), ())), preferred_element_type=F32)
            * scale
        )
        logits = jnp.where(valid, logits, -1e30)
        top = jnp.max(logits, axis=-1, keepdims=True)
        weights = jnp.exp(logits - top)
        total = jnp.sum(weights, axis=-1, keepdims=True)
        summed = jnp.dot(weights.astype(BF16), values, preferred_element_type=F32)
        result[...] = summed / total
        for g in range(CHILDREN * pairs):
            item[j, g] = result[g * PAIR : (g + 1) * PAIR, :].astype(BF16)
        log_total = top + jnp.log(total)
        tails = []
        for c in range(CHILDREN):
            parts = in_parts(jnp.broadcast_to(log_total[c * rows : (c + 1) * rows], (rows, HD)))
            chosen = jnp.where(
                lane < rows, parts[0], jnp.where(lane < 2 * rows, parts[1], parts[2])
            )
            line = jnp.sum(jnp.where(diagonal, chosen, 0.0), axis=0, keepdims=True)
            for n, extra in enumerate([jnp.full((1, HD), found[1 + c].astype(F32), F32), *score]):
                line = jnp.where(part == 3 * rows + n, extra, line)
            tails.append(line)
        item[j, CHILDREN * pairs] = jnp.concatenate(tails, axis=0).astype(BF16)
    for b in range(blocks):
        out_ref[b * kv_heads : (b + 1) * kv_heads] = item[...]


def back_kernel(columns, in_ref, out_ref):
    pairs = out_ref.shape[1] - 1
    rows = pairs * PAIR
    first = lax.axis_index("zh") * out_ref.shape[0]
    children = []
    for i in range(in_ref.shape[0]):
        tail = in_ref[i, CHILDREN * pairs].astype(F32)
        children.append([whole_number(tail[c : c + 1], 3 * rows) for c in range(CHILDREN)])
    for i in range(in_ref.shape[0]):
        for c in range(CHILDREN):
            place = children[i][c] - first

            @pl.when((place >= 0) & (place < out_ref.shape[0]))
            def _():
                out_ref[place, :pairs] = in_ref[i, c * pairs : (c + 1) * pairs]
                tail = in_ref[i, CHILDREN * pairs].astype(F32)[c : c + 1]
                out_ref[place, pairs] = jnp.broadcast_to(tail, (PAIR, HD)).astype(BF16)


def merge_kernel(
    columns, facts_ref, in_ref, q_ref, nk_ref, nv_ref, rw_ref, out_ref, reward_ref, spare_ref, wide, came
):
    pairs = in_ref.shape[1] - 1
    rows = pairs * PAIR
    steps, heads = q_ref.shape[1], q_ref.shape[2] // HD
    kv_heads = nk_ref.shape[2] // HD
    size = steps * heads
    column = whole_number(facts_ref[0:1, :], 0) % columns
    lane = lax.broadcasted_iota(jnp.int32, (rows, HD), 1)
    own = lane % rows == lax.broadcasted_iota(jnp.int32, (rows, HD), 0)
    own = own & (lane < 3 * rows)
    tops = []
    for j in range(kv_heads):
        for g in range(pairs):
            came[j * rows + g * PAIR : j * rows + (g + 1) * PAIR, :] = in_ref[j * columns + column, g].astype(F32)
        tail = in_ref[j * columns + column, pairs].astype(F32)[0:1]
        tops.append(jnp.sum(jnp.where(own, tail, 0.0), axis=-1, keepdims=True))
        if j == 0:
            base = 3 * rows + 1
            inherited = (tail[:, base : base + 1] + tail[:, base + 1 : base + 2]) + tail[:, base + 2 : base + 3]
            spare_ref[...] = jnp.broadcast_to(inherited, spare_ref.shape)
    sum_parent = came[...]
    top_parent = jnp.concatenate(tops, axis=0)
    for h in range(heads):
        wide[h * steps : (h + 1) * steps, :] = q_ref[0, :, h * HD : (h + 1) * HD].astype(F32)
    query = wide[...]
    step = lax.broadcasted_iota(jnp.int32, (size, 1), 0) % steps

    def spread(ref, u):
        return jnp.concatenate(
            [
                jnp.broadcast_to(ref[0, u : u + 1, k * HD : (k + 1) * HD].astype(F32), (rows, HD))
                for k in range(kv_heads)
            ],
            axis=0,
        )

    scale = HD**-0.5
    logits = [
        jnp.where(u <= step, jnp.sum(query * spread(nk_ref, u), axis=-1, keepdims=True) * scale, -1e30)
        for u in range(steps)
    ]
    top_own = functools.reduce(jnp.maximum, logits)
    weights = [jnp.exp(x - top_own) for x in logits]
    total_own = functools.reduce(jnp.add, weights)
    sum_own = functools.reduce(
        jnp.add, [w.astype(BF16).astype(F32) * spread(nv_ref, u) for u, w in enumerate(weights)]
    )
    top = jnp.maximum(top_parent, top_own)
    factor_parent = jnp.exp(top_parent - top)
    factor_own = jnp.exp(top_own - top)
    merged = (sum_parent * factor_parent + sum_own * factor_own) / (
        factor_parent + total_own * factor_own
    )
    attended = merged.astype(BF16).astype(F32)
    wide[...] = attended
    reward = jnp.zeros((steps, HD), F32)
    for h in range(heads):
        part = wide[h * steps : (h + 1) * steps, :]
        out_ref[0, :, h * HD : (h + 1) * HD] = part.astype(BF16)
        reward = reward + part * rw_ref[h * HD : (h + 1) * HD].astype(F32)[None, :]
    reward_ref[...] = jnp.broadcast_to(jnp.sum(reward, axis=-1, keepdims=True), reward_ref.shape)


def per_device(
    cache_keys,
    cache_values,
    lengths,
    parent_scores,
    parents,
    queries,
    new_keys,
    new_values,
    reward_weight,
):
    columns = lax.axis_size("x")
    near, far = lax.axis_size(NEAR), lax.axis_size(FAR)
    steps, width = queries.shape[1:]
    heads = width // HD
    kv_heads = cache_keys.shape[2] // HD
    size = steps * heads
    rows = size // kv_heads
    pairs = rows // PAIR
    one, both = (pairs + 1, PAIR, HD), (CHILDREN * pairs + 1, PAIR, HD)

    def array(*shape, kind=BF16):
        return jax.ShapeDtypeStruct(shape, kind)

    sent, facts = pl.pallas_call(
        functools.partial(send_kernel, columns),
        out_shape=(array(near, *one), array(TILE, HD, kind=F32)),
        in_specs=[SMEM, SMEM, SMEM, VMEM],
        out_specs=(VMEM, VMEM),
        compiler_params=limit(4),
        cost_estimate=SLOW,
        name="send",
    )(parents, lengths, parent_scores, queries)
    pieces = lax.all_to_all(sent, NEAR, 0, 0, tiled=True)
    turned = pl.pallas_call(
        functools.partial(turn_kernel, columns),
        out_shape=array(far, *both),
        in_specs=[VMEM],
        out_specs=VMEM,
        scratch_shapes=[pltpu.SMEM((far,), jnp.int32), pltpu.VMEM((far, TILE, HD), F32)],
        compiler_params=limit(4),
        cost_estimate=SLOW,
        name="turn",
    )(pieces)
    asked = lax.all_to_all(turned, FAR, 0, 0, tiled=True)
    outputs = pl.pallas_call(
        attend_kernel,
        out_shape=array(far, *both),
        in_specs=[VMEM, VMEM, VMEM, VMEM],
        out_specs=VMEM,
        scratch_shapes=[
            pltpu.VMEM((kv_heads, CHILDREN, rows, HD), F32),
            pltpu.VMEM((CHILDREN * rows, HD), F32),
            pltpu.VMEM((kv_heads, *both), BF16),
            pltpu.SMEM((1 + CHILDREN,), jnp.int32),
        ],
        compiler_params=limit(16),
        name="attend",
    )(facts, asked, cache_keys, cache_values)
    answers = lax.all_to_all(outputs, FAR, 0, 0, tiled=True)
    back = pl.pallas_call(
        functools.partial(back_kernel, columns),
        out_shape=array(near, *one),
        in_specs=[VMEM],
        out_specs=VMEM,
        compiler_params=limit(4),
        name="back",
    )(answers)
    pieces = lax.all_to_all(back, NEAR, 0, 0, tiled=True)
    output, partial_reward, inherited = pl.pallas_call(
        functools.partial(merge_kernel, columns),
        out_shape=(
            array(*queries.shape),
            array(steps, HD, kind=F32),
            array(1, HD, kind=F32),
        ),
        in_specs=[VMEM, VMEM, VMEM, VMEM, VMEM, VMEM],
        out_specs=(VMEM, VMEM, VMEM),
        scratch_shapes=[pltpu.VMEM((size, HD), F32), pltpu.VMEM((size, HD), F32)],
        compiler_params=limit(4),
        name="merge",
    )(facts, pieces, queries, new_keys, new_values, reward_weight)
    reward = lax.psum(partial_reward, "tensor")[:, 0]
    score = inherited[0, :1] + jnp.sum(jax.nn.log_sigmoid(reward))
    return (output, score)


def solution(mesh):
    finer = Mesh(
        mesh.devices.reshape(mesh.shape["groups"], 4, 4, 8, mesh.shape["tensor"]),
        ("groups", "zh", "zl", "x", "tensor"),
    )
    return jax.shard_map(
        per_device,
        mesh=finer,
        in_specs=(
            P(GROUPS_DP, None, "tensor"),
            P(GROUPS_DP, None, "tensor"),
            P(GROUPS_DP),
            P(GROUPS_DP),
            P(GROUPS_DP),
            P(GROUPS_DP, None, "tensor"),
            P(GROUPS_DP, None, "tensor"),
            P(GROUPS_DP, None, "tensor"),
            P("tensor"),
        ),
        out_specs=(P(GROUPS_DP, None, "tensor"), P(GROUPS_DP)),
        check_vma=False,
    )
```

```python
import functools

import jax
import jax.numpy as jnp
from jax import lax
from jax.experimental import pallas as pl
from jax.experimental.pallas import tpu as pltpu
from jax.sharding import Mesh
from jax.sharding import PartitionSpec as P

HD = 128
CHILDREN = 2
PAIR = 2
TILE = 8
GROUPS_DP = ("groups", "zh", "zl", "x")
NEAR = ("zl", "x")
FAR = ("zh", "zl")
VMEM = pl.BlockSpec(memory_space=pltpu.VMEM)
SMEM = pl.BlockSpec(memory_space=pltpu.SMEM)
BF16 = jnp.bfloat16
F32 = jnp.float32
SLOW = pl.CostEstimate(flops=10**10, bytes_accessed=2**26, transcendentals=0)


def limit(mib):
    return pltpu.CompilerParams(vmem_limit_bytes=mib * 1024 * 1024)


def whole_number(row, lane):
    return jnp.sum(row[:, lane : lane + 1]).astype(jnp.int32)


def in_parts(x):
    first = x.astype(BF16)
    rest = x - first.astype(F32)
    second = rest.astype(BF16)
    third = (rest - second.astype(F32)).astype(BF16)
    return [part.astype(F32) for part in (first, second, third)]


def send_kernel(kv_heads, parents_ref, lengths_ref, scores_ref, q_ref, out_ref, facts_ref):
    steps = q_ref.shape[1]
    pairs = out_ref.shape[1] - 1
    turns = steps // PAIR
    facts = [parents_ref[0].astype(F32), lengths_ref[0].astype(F32), scores_ref[0]]
    for n, fact in enumerate(facts):
        facts_ref[n : n + 1, :] = jnp.full((1, HD), fact, F32)
    parent = jnp.full((PAIR, HD), facts[0], F32).astype(BF16)
    for j in range(kv_heads):
        for g in range(pairs):
            h, t = j * (pairs // turns) + g // turns, g % turns * PAIR
            pair = q_ref[0, t : t + PAIR, h * HD : (h + 1) * HD]
            for d in range(j, out_ref.shape[0], kv_heads):
                out_ref[d, g] = pair
        for d in range(j, out_ref.shape[0], kv_heads):
            out_ref[d, pairs] = parent


def turn_kernel(columns, in_ref, out_ref, used, meta):
    pairs = in_ref.shape[1] - 1
    first = lax.axis_index("zh") * out_ref.shape[0]
    mine = lax.axis_index("x")
    parents = [whole_number(in_ref[i, pairs].astype(F32)[0:1], 0) for i in range(in_ref.shape[0])]
    meta[...] = jnp.full(meta.shape, -1.0, F32)
    for i in range(out_ref.shape[0]):
        used[i] = 0
    for i, parent in enumerate(parents):
        place = parent - first

        @pl.when((place >= 0) & (place < out_ref.shape[0]))
        def _():
            n = used[place]
            used[place] = n + 1
            out_ref[place, pl.ds(n * pairs, pairs)] = in_ref[i, :pairs]
            child = i * columns + mine
            meta[place, pl.ds(n, 1), :] = jnp.full((1, HD), child.astype(F32), F32)

    for i in range(out_ref.shape[0]):
        out_ref[i, CHILDREN * pairs] = meta[i, :CHILDREN, :].astype(BF16)


def attend_kernel(facts_ref, in_ref, k_ref, v_ref, out_ref, q, result, item, found):
    kv_heads = item.shape[0]
    pairs = in_ref.shape[1] // CHILDREN
    rows = pairs * PAIR
    context = k_ref.shape[1]
    columns = in_ref.shape[0] // kv_heads
    ids = []
    for b in range(columns):
        tail = in_ref[b, CHILDREN * pairs].astype(F32)
        ids.append([whole_number(tail[c : c + 1], 0) for c in range(CHILDREN)])
    q[...] = jnp.zeros_like(q)
    found[0] = 0
    for c in range(CHILDREN):
        found[1 + c] = -1
    for b in range(columns):
        for c in range(CHILDREN):

            @pl.when(ids[b][c] >= 0)
            def _():
                n = found[0]
                found[0] = n + 1
                found[1 + n] = ids[b][c]
                for j in range(kv_heads):
                    for g in range(pairs):
                        pair = in_ref[j * columns + b, c * pairs + g].astype(F32)
                        q[j, n, g * PAIR : (g + 1) * PAIR, :] = pair

    scale = HD**-0.5
    length = facts_ref[1:2, 0:1].astype(jnp.int32)
    valid = lax.broadcasted_iota(jnp.int32, (CHILDREN * rows, context), 1) < length
    lane = lax.broadcasted_iota(jnp.int32, (rows, HD), 1)
    diagonal = lane % rows == lax.broadcasted_iota(jnp.int32, (rows, HD), 0)
    part = lax.broadcasted_iota(jnp.int32, (1, HD), 1)
    score = in_parts(facts_ref[2:3, :])
    for j in range(kv_heads):
        keys = k_ref[0, :, j * HD : (j + 1) * HD]
        values = v_ref[0, :, j * HD : (j + 1) * HD]
        query = q[j].reshape(CHILDREN * rows, HD).astype(BF16)
        logits = (
            lax.dot_general(query, keys, (((1,), (1,)), ((), ())), preferred_element_type=F32)
            * scale
        )
        logits = jnp.where(valid, logits, -1e30)
        top = jnp.max(logits, axis=-1, keepdims=True)
        weights = jnp.exp(logits - top)
        total = jnp.sum(weights, axis=-1, keepdims=True)
        summed = jnp.dot(weights.astype(BF16), values, preferred_element_type=F32)
        result[...] = summed / total
        for g in range(CHILDREN * pairs):
            item[j, g] = result[g * PAIR : (g + 1) * PAIR, :].astype(BF16)
        log_total = top + jnp.log(total)
        tails = []
        for c in range(CHILDREN):
            parts = in_parts(jnp.broadcast_to(log_total[c * rows : (c + 1) * rows], (rows, HD)))
            chosen = jnp.where(
                lane < rows, parts[0], jnp.where(lane < 2 * rows, parts[1], parts[2])
            )
            line = jnp.sum(jnp.where(diagonal, chosen, 0.0), axis=0, keepdims=True)
            for n, extra in enumerate([jnp.full((1, HD), found[1 + c].astype(F32), F32), *score]):
                line = jnp.where(part == 3 * rows + n, extra, line)
            tails.append(line)
        item[j, CHILDREN * pairs] = jnp.concatenate(tails, axis=0).astype(BF16)
    for b in range(out_ref.shape[0] // kv_heads):
        out_ref[b * kv_heads : (b + 1) * kv_heads] = item[...]


def back_kernel(columns, in_ref, out_ref):
    pairs = out_ref.shape[1] - 1
    rows = pairs * PAIR
    first = lax.axis_index("zh") * out_ref.shape[0]
    children = []
    for i in range(in_ref.shape[0]):
        tail = in_ref[i, CHILDREN * pairs].astype(F32)
        children.append([whole_number(tail[c : c + 1], 3 * rows) for c in range(CHILDREN)])
    for i in range(in_ref.shape[0]):
        for c in range(CHILDREN):
            place = children[i][c] - first

            @pl.when((place >= 0) & (place < out_ref.shape[0]))
            def _():
                out_ref[place, :pairs] = in_ref[i, c * pairs : (c + 1) * pairs]
                tail = in_ref[i, CHILDREN * pairs].astype(F32)[c : c + 1]
                out_ref[place, pairs] = jnp.broadcast_to(tail, (PAIR, HD)).astype(BF16)


def merge_kernel(
    columns, facts_ref, in_ref, q_ref, nk_ref, nv_ref, rw_ref, out_ref, reward_ref, spare_ref, wide, came
):
    pairs = in_ref.shape[1] - 1
    rows = pairs * PAIR
    steps, heads = q_ref.shape[1], q_ref.shape[2] // HD
    kv_heads = nk_ref.shape[2] // HD
    size = steps * heads
    column = whole_number(facts_ref[0:1, :], 0) % columns
    lane = lax.broadcasted_iota(jnp.int32, (rows, HD), 1)
    own = lane % rows == lax.broadcasted_iota(jnp.int32, (rows, HD), 0)
    own = own & (lane < 3 * rows)
    tops = []
    for j in range(kv_heads):
        for g in range(pairs):
            came[j * rows + g * PAIR : j * rows + (g + 1) * PAIR, :] = in_ref[j * columns + column, g].astype(F32)
        tail = in_ref[j * columns + column, pairs].astype(F32)[0:1]
        tops.append(jnp.sum(jnp.where(own, tail, 0.0), axis=-1, keepdims=True))
        if j == 0:
            base = 3 * rows + 1
            inherited = (tail[:, base : base + 1] + tail[:, base + 1 : base + 2]) + tail[:, base + 2 : base + 3]
            spare_ref[...] = jnp.broadcast_to(inherited, spare_ref.shape)
    sum_parent = came[...]
    top_parent = jnp.concatenate(tops, axis=0)
    for h in range(heads):
        wide[h * steps : (h + 1) * steps, :] = q_ref[0, :, h * HD : (h + 1) * HD].astype(F32)
    query = wide[...]
    step = lax.broadcasted_iota(jnp.int32, (size, 1), 0) % steps

    def spread(ref, u):
        return jnp.concatenate(
            [
                jnp.broadcast_to(ref[0, u : u + 1, k * HD : (k + 1) * HD].astype(F32), (rows, HD))
                for k in range(kv_heads)
            ],
            axis=0,
        )

    scale = HD**-0.5
    logits = [
        jnp.where(u <= step, jnp.sum(query * spread(nk_ref, u), axis=-1, keepdims=True) * scale, -1e30)
        for u in range(steps)
    ]
    top_own = functools.reduce(jnp.maximum, logits)
    weights = [jnp.exp(x - top_own) for x in logits]
    total_own = functools.reduce(jnp.add, weights)
    sum_own = functools.reduce(
        jnp.add, [w.astype(BF16).astype(F32) * spread(nv_ref, u) for u, w in enumerate(weights)]
    )
    top = jnp.maximum(top_parent, top_own)
    factor_parent = jnp.exp(top_parent - top)
    factor_own = jnp.exp(top_own - top)
    merged = (sum_parent * factor_parent + sum_own * factor_own) / (
        factor_parent + total_own * factor_own
    )
    attended = merged.astype(BF16).astype(F32)
    wide[...] = attended
    reward = jnp.zeros((steps, HD), F32)
    for h in range(heads):
        part = wide[h * steps : (h + 1) * steps, :]
        out_ref[0, :, h * HD : (h + 1) * HD] = part.astype(BF16)
        reward = reward + part * rw_ref[h * HD : (h + 1) * HD].astype(F32)[None, :]
    reward_ref[...] = jnp.broadcast_to(jnp.sum(reward, axis=-1, keepdims=True), reward_ref.shape)


def per_device(
    cache_keys,
    cache_values,
    lengths,
    parent_scores,
    parents,
    queries,
    new_keys,
    new_values,
    reward_weight,
):
    columns = lax.axis_size("x")
    near, far = lax.axis_size(NEAR), lax.axis_size(FAR)
    steps, width = queries.shape[1:]
    heads = width // HD
    kv_heads = cache_keys.shape[2] // HD
    size = steps * heads
    rows = size // kv_heads
    pairs = rows // PAIR
    one, both = (pairs + 1, PAIR, HD), (CHILDREN * pairs + 1, PAIR, HD)

    def array(*shape, kind=BF16):
        return jax.ShapeDtypeStruct(shape, kind)

    sent, facts = pl.pallas_call(
        functools.partial(send_kernel, kv_heads),
        out_shape=(array(far, *one), array(TILE, HD, kind=F32)),
        in_specs=[SMEM, SMEM, SMEM, VMEM],
        out_specs=(VMEM, VMEM),
        compiler_params=limit(4),
        cost_estimate=SLOW,
        name="send",
    )(parents, lengths, parent_scores, queries)
    pieces = lax.all_to_all(sent, FAR, 0, 0, tiled=True)
    turned = pl.pallas_call(
        functools.partial(turn_kernel, columns),
        out_shape=array(near, *both),
        in_specs=[VMEM],
        out_specs=VMEM,
        scratch_shapes=[pltpu.SMEM((near,), jnp.int32), pltpu.VMEM((near, TILE, HD), F32)],
        compiler_params=limit(4),
        cost_estimate=SLOW,
        name="turn",
    )(pieces)
    asked = lax.all_to_all(turned, NEAR, 0, 0, tiled=True)
    outputs = pl.pallas_call(
        attend_kernel,
        out_shape=array(far, *both),
        in_specs=[VMEM, VMEM, VMEM, VMEM],
        out_specs=VMEM,
        scratch_shapes=[
            pltpu.VMEM((kv_heads, CHILDREN, rows, HD), F32),
            pltpu.VMEM((CHILDREN * rows, HD), F32),
            pltpu.VMEM((kv_heads, *both), BF16),
            pltpu.SMEM((1 + CHILDREN,), jnp.int32),
        ],
        compiler_params=limit(16),
        name="attend",
    )(facts, asked, cache_keys, cache_values)
    answers = lax.all_to_all(outputs, FAR, 0, 0, tiled=True)
    back = pl.pallas_call(
        functools.partial(back_kernel, columns),
        out_shape=array(near, *one),
        in_specs=[VMEM],
        out_specs=VMEM,
        compiler_params=limit(4),
        name="back",
    )(answers)
    pieces = lax.all_to_all(back, NEAR, 0, 0, tiled=True)
    output, partial_reward, inherited = pl.pallas_call(
        functools.partial(merge_kernel, columns),
        out_shape=(
            array(*queries.shape),
            array(steps, HD, kind=F32),
            array(1, HD, kind=F32),
        ),
        in_specs=[VMEM, VMEM, VMEM, VMEM, VMEM, VMEM],
        out_specs=(VMEM, VMEM, VMEM),
        scratch_shapes=[pltpu.VMEM((size, HD), F32), pltpu.VMEM((size, HD), F32)],
        compiler_params=limit(4),
        name="merge",
    )(facts, pieces, queries, new_keys, new_values, reward_weight)
    reward = lax.psum(partial_reward, "tensor")[:, 0]
    score = inherited[0, :1] + jnp.sum(jax.nn.log_sigmoid(reward))
    return (output, score)


def solution(mesh):
    finer = Mesh(
        mesh.devices.reshape(mesh.shape["groups"], 4, 4, 8, mesh.shape["tensor"]),
        ("groups", "zh", "zl", "x", "tensor"),
    )
    return jax.shard_map(
        per_device,
        mesh=finer,
        in_specs=(
            P(GROUPS_DP, None, "tensor"),
            P(GROUPS_DP, None, "tensor"),
            P(GROUPS_DP),
            P(GROUPS_DP),
            P(GROUPS_DP),
            P(GROUPS_DP, None, "tensor"),
            P(GROUPS_DP, None, "tensor"),
            P(GROUPS_DP, None, "tensor"),
            P("tensor"),
        ),
        out_specs=(P(GROUPS_DP, None, "tensor"), P(GROUPS_DP)),
        check_vma=False,
    )
```

```python
import functools

import jax
import jax.numpy as jnp
from jax import lax
from jax.experimental import pallas as pl
from jax.experimental.pallas import tpu as pltpu
from jax.sharding import Mesh
from jax.sharding import PartitionSpec as P

HD = 128
CHILDREN = 2
PAIR = 2
TILE = 8
HEAD_START = 6000
GROUPS_DP = ("groups", "zh", "zl", "x")
NEAR = ("zl", "x")
FAR = ("zh", "zl")
VMEM = pl.BlockSpec(memory_space=pltpu.VMEM)
SMEM = pl.BlockSpec(memory_space=pltpu.SMEM)
BF16 = jnp.bfloat16
F32 = jnp.float32
SLOW = pl.CostEstimate(flops=10**10, bytes_accessed=2**26, transcendentals=0)


def limit(mib):
    return pltpu.CompilerParams(vmem_limit_bytes=mib * 1024 * 1024)


def whole_number(row, lane):
    return jnp.sum(row[:, lane : lane + 1]).astype(jnp.int32)


def in_parts(x):
    first = x.astype(BF16)
    rest = x - first.astype(F32)
    second = rest.astype(BF16)
    third = (rest - second.astype(F32)).astype(BF16)
    return [part.astype(F32) for part in (first, second, third)]


def send_kernel(columns, parents_ref, lengths_ref, scores_ref, q_ref, out_ref, facts_ref):
    steps = q_ref.shape[1]
    pairs = out_ref.shape[1] - 1
    turns = steps // PAIR
    @pl.when(lax.axis_index("tensor") == 1)
    def _():
        pl.delay(HEAD_START)

    facts = [parents_ref[0].astype(F32), lengths_ref[0].astype(F32), scores_ref[0]]
    for n, fact in enumerate(facts):
        facts_ref[n : n + 1, :] = jnp.full((1, HD), fact, F32)
    parent = jnp.full((PAIR, HD), facts[0], F32).astype(BF16)
    for j in range(out_ref.shape[0] // columns):
        for g in range(pairs):
            h, t = j * (pairs // turns) + g // turns, g % turns * PAIR
            pair = q_ref[0, t : t + PAIR, h * HD : (h + 1) * HD]
            for d in range(columns):
                out_ref[j * columns + d, g] = pair
        for d in range(columns):
            out_ref[j * columns + d, pairs] = parent


def turn_kernel(columns, in_ref, out_ref, used, meta):
    pairs = in_ref.shape[1] - 1
    block = in_ref.shape[0] // columns
    first = lax.axis_index("zh") * block
    mine = lax.axis_index("x")
    parents = [whole_number(in_ref[i, pairs].astype(F32)[0:1], 0) for i in range(in_ref.shape[0])]
    meta[...] = jnp.full(meta.shape, -1.0, F32)
    for i in range(out_ref.shape[0]):
        used[i] = 0
    for i, parent in enumerate(parents):

        @pl.when(parent % columns == mine)
        def _():
            row = parent // columns
            place = used[row]
            used[row] = place + 1
            out_ref[row, pl.ds(place * pairs, pairs)] = in_ref[i, :pairs]
            child = first * columns + i
            meta[row, pl.ds(place, 1), :] = jnp.full((1, HD), child.astype(F32), F32)

    for i in range(out_ref.shape[0]):
        out_ref[i, CHILDREN * pairs] = meta[i, :CHILDREN, :].astype(BF16)


def attend_kernel(facts_ref, in_ref, k_ref, v_ref, out_ref, q, result, item, found):
    kv_heads = item.shape[0]
    pairs = in_ref.shape[1] // CHILDREN
    rows = pairs * PAIR
    context = k_ref.shape[1]
    blocks = in_ref.shape[0] // kv_heads
    ids = []
    for b in range(blocks):
        tail = in_ref[b * kv_heads, CHILDREN * pairs].astype(F32)
        ids.append([whole_number(tail[c : c + 1], 0) for c in range(CHILDREN)])
    q[...] = jnp.zeros_like(q)
    found[0] = 0
    for c in range(CHILDREN):
        found[1 + c] = -1
    for b in range(blocks):
        for c in range(CHILDREN):

            @pl.when(ids[b][c] >= 0)
            def _():
                n = found[0]
                found[0] = n + 1
                found[1 + n] = ids[b][c]
                for j in range(kv_heads):
                    for g in range(pairs):
                        pair = in_ref[b * kv_heads + j, c * pairs + g].astype(F32)
                        q[j, n, g * PAIR : (g + 1) * PAIR, :] = pair

    scale = HD**-0.5
    length = facts_ref[1:2, 0:1].astype(jnp.int32)
    valid = lax.broadcasted_iota(jnp.int32, (CHILDREN * rows, context), 1) < length
    lane = lax.broadcasted_iota(jnp.int32, (rows, HD), 1)
    diagonal = lane % rows == lax.broadcasted_iota(jnp.int32, (rows, HD), 0)
    part = lax.broadcasted_iota(jnp.int32, (1, HD), 1)
    score = in_parts(facts_ref[2:3, :])
    for j in range(kv_heads):
        keys = k_ref[0, :, j * HD : (j + 1) * HD]
        values = v_ref[0, :, j * HD : (j + 1) * HD]
        query = q[j].reshape(CHILDREN * rows, HD).astype(BF16)
        logits = (
            lax.dot_general(query, keys, (((1,), (1,)), ((), ())), preferred_element_type=F32)
            * scale
        )
        logits = jnp.where(valid, logits, -1e30)
        top = jnp.max(logits, axis=-1, keepdims=True)
        weights = jnp.exp(logits - top)
        total = jnp.sum(weights, axis=-1, keepdims=True)
        summed = jnp.dot(weights.astype(BF16), values, preferred_element_type=F32)
        result[...] = summed / total
        for g in range(CHILDREN * pairs):
            item[j, g] = result[g * PAIR : (g + 1) * PAIR, :].astype(BF16)
        log_total = top + jnp.log(total)
        tails = []
        for c in range(CHILDREN):
            parts = in_parts(jnp.broadcast_to(log_total[c * rows : (c + 1) * rows], (rows, HD)))
            chosen = jnp.where(
                lane < rows, parts[0], jnp.where(lane < 2 * rows, parts[1], parts[2])
            )
            line = jnp.sum(jnp.where(diagonal, chosen, 0.0), axis=0, keepdims=True)
            for n, extra in enumerate([jnp.full((1, HD), found[1 + c].astype(F32), F32), *score]):
                line = jnp.where(part == 3 * rows + n, extra, line)
            tails.append(line)
        item[j, CHILDREN * pairs] = jnp.concatenate(tails, axis=0).astype(BF16)
    for b in range(blocks):
        out_ref[b * kv_heads : (b + 1) * kv_heads] = item[...]


def back_kernel(columns, in_ref, out_ref):
    pairs = out_ref.shape[1] - 1
    rows = pairs * PAIR
    first = lax.axis_index("zh") * out_ref.shape[0]
    children = []
    for i in range(in_ref.shape[0]):
        tail = in_ref[i, CHILDREN * pairs].astype(F32)
        children.append([whole_number(tail[c : c + 1], 3 * rows) for c in range(CHILDREN)])
    for i in range(in_ref.shape[0]):
        for c in range(CHILDREN):
            place = children[i][c] - first

            @pl.when((place >= 0) & (place < out_ref.shape[0]))
            def _():
                out_ref[place, :pairs] = in_ref[i, c * pairs : (c + 1) * pairs]
                tail = in_ref[i, CHILDREN * pairs].astype(F32)[c : c + 1]
                out_ref[place, pairs] = jnp.broadcast_to(tail, (PAIR, HD)).astype(BF16)


def merge_kernel(
    columns, facts_ref, in_ref, q_ref, nk_ref, nv_ref, rw_ref, out_ref, reward_ref, spare_ref, wide, came
):
    pairs = in_ref.shape[1] - 1
    rows = pairs * PAIR
    steps, heads = q_ref.shape[1], q_ref.shape[2] // HD
    kv_heads = nk_ref.shape[2] // HD
    size = steps * heads
    column = whole_number(facts_ref[0:1, :], 0) % columns
    lane = lax.broadcasted_iota(jnp.int32, (rows, HD), 1)
    own = lane % rows == lax.broadcasted_iota(jnp.int32, (rows, HD), 0)
    own = own & (lane < 3 * rows)
    tops = []
    for j in range(kv_heads):
        for g in range(pairs):
            came[j * rows + g * PAIR : j * rows + (g + 1) * PAIR, :] = in_ref[j * columns + column, g].astype(F32)
        tail = in_ref[j * columns + column, pairs].astype(F32)[0:1]
        tops.append(jnp.sum(jnp.where(own, tail, 0.0), axis=-1, keepdims=True))
        if j == 0:
            base = 3 * rows + 1
            inherited = (tail[:, base : base + 1] + tail[:, base + 1 : base + 2]) + tail[:, base + 2 : base + 3]
            spare_ref[...] = jnp.broadcast_to(inherited, spare_ref.shape)
    sum_parent = came[...]
    top_parent = jnp.concatenate(tops, axis=0)
    for h in range(heads):
        wide[h * steps : (h + 1) * steps, :] = q_ref[0, :, h * HD : (h + 1) * HD].astype(F32)
    query = wide[...]
    step = lax.broadcasted_iota(jnp.int32, (size, 1), 0) % steps

    def spread(ref, u):
        return jnp.concatenate(
            [
                jnp.broadcast_to(ref[0, u : u + 1, k * HD : (k + 1) * HD].astype(F32), (rows, HD))
                for k in range(kv_heads)
            ],
            axis=0,
        )

    scale = HD**-0.5
    logits = [
        jnp.where(u <= step, jnp.sum(query * spread(nk_ref, u), axis=-1, keepdims=True) * scale, -1e30)
        for u in range(steps)
    ]
    top_own = functools.reduce(jnp.maximum, logits)
    weights = [jnp.exp(x - top_own) for x in logits]
    total_own = functools.reduce(jnp.add, weights)
    sum_own = functools.reduce(
        jnp.add, [w.astype(BF16).astype(F32) * spread(nv_ref, u) for u, w in enumerate(weights)]
    )
    top = jnp.maximum(top_parent, top_own)
    factor_parent = jnp.exp(top_parent - top)
    factor_own = jnp.exp(top_own - top)
    merged = (sum_parent * factor_parent + sum_own * factor_own) / (
        factor_parent + total_own * factor_own
    )
    attended = merged.astype(BF16).astype(F32)
    wide[...] = attended
    reward = jnp.zeros((steps, HD), F32)
    for h in range(heads):
        part = wide[h * steps : (h + 1) * steps, :]
        out_ref[0, :, h * HD : (h + 1) * HD] = part.astype(BF16)
        reward = reward + part * rw_ref[h * HD : (h + 1) * HD].astype(F32)[None, :]
    reward_ref[...] = jnp.broadcast_to(jnp.sum(reward, axis=-1, keepdims=True), reward_ref.shape)


def per_device(
    cache_keys,
    cache_values,
    lengths,
    parent_scores,
    parents,
    queries,
    new_keys,
    new_values,
    reward_weight,
):
    columns = lax.axis_size("x")
    near, far = lax.axis_size(NEAR), lax.axis_size(FAR)
    steps, width = queries.shape[1:]
    heads = width // HD
    kv_heads = cache_keys.shape[2] // HD
    size = steps * heads
    rows = size // kv_heads
    pairs = rows // PAIR
    one, both = (pairs + 1, PAIR, HD), (CHILDREN * pairs + 1, PAIR, HD)

    def array(*shape, kind=BF16):
        return jax.ShapeDtypeStruct(shape, kind)

    sent, facts = pl.pallas_call(
        functools.partial(send_kernel, columns),
        out_shape=(array(near, *one), array(TILE, HD, kind=F32)),
        in_specs=[SMEM, SMEM, SMEM, VMEM],
        out_specs=(VMEM, VMEM),
        compiler_params=limit(4),
        cost_estimate=SLOW,
        name="send",
    )(parents, lengths, parent_scores, queries)
    pieces = lax.all_to_all(sent, NEAR, 0, 0, tiled=True)
    turned = pl.pallas_call(
        functools.partial(turn_kernel, columns),
        out_shape=array(far, *both),
        in_specs=[VMEM],
        out_specs=VMEM,
        scratch_shapes=[pltpu.SMEM((far,), jnp.int32), pltpu.VMEM((far, TILE, HD), F32)],
        compiler_params=limit(4),
        cost_estimate=SLOW,
        name="turn",
    )(pieces)
    asked = lax.all_to_all(turned, FAR, 0, 0, tiled=True)
    outputs = pl.pallas_call(
        attend_kernel,
        out_shape=array(far, *both),
        in_specs=[VMEM, VMEM, VMEM, VMEM],
        out_specs=VMEM,
        scratch_shapes=[
            pltpu.VMEM((kv_heads, CHILDREN, rows, HD), F32),
            pltpu.VMEM((CHILDREN * rows, HD), F32),
            pltpu.VMEM((kv_heads, *both), BF16),
            pltpu.SMEM((1 + CHILDREN,), jnp.int32),
        ],
        compiler_params=limit(16),
        name="attend",
    )(facts, asked, cache_keys, cache_values)
    answers = lax.all_to_all(outputs, FAR, 0, 0, tiled=True)
    back = pl.pallas_call(
        functools.partial(back_kernel, columns),
        out_shape=array(near, *one),
        in_specs=[VMEM],
        out_specs=VMEM,
        compiler_params=limit(4),
        name="back",
    )(answers)
    pieces = lax.all_to_all(back, NEAR, 0, 0, tiled=True)
    output, partial_reward, inherited = pl.pallas_call(
        functools.partial(merge_kernel, columns),
        out_shape=(
            array(*queries.shape),
            array(steps, HD, kind=F32),
            array(1, HD, kind=F32),
        ),
        in_specs=[VMEM, VMEM, VMEM, VMEM, VMEM, VMEM],
        out_specs=(VMEM, VMEM, VMEM),
        scratch_shapes=[pltpu.VMEM((size, HD), F32), pltpu.VMEM((size, HD), F32)],
        compiler_params=limit(4),
        name="merge",
    )(facts, pieces, queries, new_keys, new_values, reward_weight)
    reward = lax.psum(partial_reward, "tensor")[:, 0]
    score = inherited[0, :1] + jnp.sum(jax.nn.log_sigmoid(reward))
    return (output, score)


def solution(mesh):
    finer = Mesh(
        mesh.devices.reshape(mesh.shape["groups"], 4, 4, 8, mesh.shape["tensor"]),
        ("groups", "zh", "zl", "x", "tensor"),
    )
    return jax.shard_map(
        per_device,
        mesh=finer,
        in_specs=(
            P(GROUPS_DP, None, "tensor"),
            P(GROUPS_DP, None, "tensor"),
            P(GROUPS_DP),
            P(GROUPS_DP),
            P(GROUPS_DP),
            P(GROUPS_DP, None, "tensor"),
            P(GROUPS_DP, None, "tensor"),
            P(GROUPS_DP, None, "tensor"),
            P("tensor"),
        ),
        out_specs=(P(GROUPS_DP, None, "tensor"), P(GROUPS_DP)),
        check_vma=False,
    )
```

```python
import functools

import jax
import jax.numpy as jnp
from jax import lax
from jax.experimental import pallas as pl
from jax.experimental.pallas import tpu as pltpu
from jax.sharding import Mesh
from jax.sharding import PartitionSpec as P

HD = 128
CHILDREN = 2
PAIR = 2
TILE = 8
GROUPS_DP = ("groups", "zh", "zl", "x")
NEAR = ("zl", "x")
FAR = ("zh", "zl")
VMEM = pl.BlockSpec(memory_space=pltpu.VMEM)
SMEM = pl.BlockSpec(memory_space=pltpu.SMEM)
BF16 = jnp.bfloat16
F32 = jnp.float32
SLOW = pl.CostEstimate(flops=10**10, bytes_accessed=2**26, transcendentals=0)


def limit(mib):
    return pltpu.CompilerParams(vmem_limit_bytes=mib * 1024 * 1024)


def whole_number(row, lane):
    return jnp.sum(row[:, lane : lane + 1]).astype(jnp.int32)


def in_parts(x):
    first = x.astype(BF16)
    rest = x - first.astype(F32)
    second = rest.astype(BF16)
    third = (rest - second.astype(F32)).astype(BF16)
    return [part.astype(F32) for part in (first, second, third)]


def send_kernel(kv_heads, parents_ref, lengths_ref, scores_ref, q_ref, out_ref, facts_ref):
    steps = q_ref.shape[1]
    pairs = out_ref.shape[1] - 1
    turns = steps // PAIR
    facts = [parents_ref[0].astype(F32), lengths_ref[0].astype(F32), scores_ref[0]]
    for n, fact in enumerate(facts):
        facts_ref[n : n + 1, :] = jnp.full((1, HD), fact, F32)
    parent = jnp.full((PAIR, HD), facts[0], F32).astype(BF16)
    for j in range(kv_heads):
        for g in range(pairs):
            h, t = j * (pairs // turns) + g // turns, g % turns * PAIR
            pair = q_ref[0, t : t + PAIR, h * HD : (h + 1) * HD]
            for d in range(j, out_ref.shape[0], kv_heads):
                out_ref[d, g] = pair
        for d in range(j, out_ref.shape[0], kv_heads):
            out_ref[d, pairs] = parent


def turn_kernel(columns, in_ref, out_ref, used, meta):
    pairs = in_ref.shape[1] - 1
    first = lax.axis_index("zh") * out_ref.shape[0]
    mine = lax.axis_index("x")
    parents = [whole_number(in_ref[i, pairs].astype(F32)[0:1], 0) for i in range(in_ref.shape[0])]
    meta[...] = jnp.full(meta.shape, -1.0, F32)
    for i in range(out_ref.shape[0]):
        used[i] = 0
    for i, parent in enumerate(parents):
        place = parent - first

        @pl.when((place >= 0) & (place < out_ref.shape[0]))
        def _():
            n = used[place]
            used[place] = n + 1
            out_ref[place, pl.ds(n * pairs, pairs)] = in_ref[i, :pairs]
            child = i * columns + mine
            meta[place, pl.ds(n, 1), :] = jnp.full((1, HD), child.astype(F32), F32)

    for i in range(out_ref.shape[0]):
        out_ref[i, CHILDREN * pairs] = meta[i, :CHILDREN, :].astype(BF16)


def attend_kernel(facts_ref, in_ref, k_ref, v_ref, out_ref, q, result, item, found):
    kv_heads = item.shape[0]
    pairs = in_ref.shape[1] // CHILDREN
    rows = pairs * PAIR
    context = k_ref.shape[1]
    columns = in_ref.shape[0] // kv_heads
    ids = []
    for b in range(columns):
        tail = in_ref[b, CHILDREN * pairs].astype(F32)
        ids.append([whole_number(tail[c : c + 1], 0) for c in range(CHILDREN)])
    q[...] = jnp.zeros_like(q)
    found[0] = 0
    for c in range(CHILDREN):
        found[1 + c] = -1
    for b in range(columns):
        for c in range(CHILDREN):

            @pl.when(ids[b][c] >= 0)
            def _():
                n = found[0]
                found[0] = n + 1
                found[1 + n] = ids[b][c]
                for j in range(kv_heads):
                    for g in range(pairs):
                        pair = in_ref[j * columns + b, c * pairs + g].astype(F32)
                        q[j, n, g * PAIR : (g + 1) * PAIR, :] = pair

    scale = HD**-0.5
    length = facts_ref[1:2, 0:1].astype(jnp.int32)
    valid = lax.broadcasted_iota(jnp.int32, (CHILDREN * rows, context), 1) < length
    lane = lax.broadcasted_iota(jnp.int32, (rows, HD), 1)
    diagonal = lane % rows == lax.broadcasted_iota(jnp.int32, (rows, HD), 0)
    part = lax.broadcasted_iota(jnp.int32, (1, HD), 1)
    score = in_parts(facts_ref[2:3, :])
    for j in range(kv_heads):
        keys = k_ref[0, :, j * HD : (j + 1) * HD]
        values = v_ref[0, :, j * HD : (j + 1) * HD]
        query = q[j].reshape(CHILDREN * rows, HD).astype(BF16)
        logits = (
            lax.dot_general(query, keys, (((1,), (1,)), ((), ())), preferred_element_type=F32)
            * scale
        )
        logits = jnp.where(valid, logits, -1e30)
        top = jnp.max(logits, axis=-1, keepdims=True)
        weights = jnp.exp(logits - top)
        total = jnp.sum(weights, axis=-1, keepdims=True)
        summed = jnp.dot(weights.astype(BF16), values, preferred_element_type=F32)
        result[...] = summed / total
        for g in range(CHILDREN * pairs):
            item[j, g] = result[g * PAIR : (g + 1) * PAIR, :].astype(BF16)
        log_total = top + jnp.log(total)
        tails = []
        for c in range(CHILDREN):
            parts = in_parts(jnp.broadcast_to(log_total[c * rows : (c + 1) * rows], (rows, HD)))
            chosen = jnp.where(
                lane < rows, parts[0], jnp.where(lane < 2 * rows, parts[1], parts[2])
            )
            line = jnp.sum(jnp.where(diagonal, chosen, 0.0), axis=0, keepdims=True)
            for n, extra in enumerate([jnp.full((1, HD), found[1 + c].astype(F32), F32), *score]):
                line = jnp.where(part == 3 * rows + n, extra, line)
            tails.append(line)
        item[j, CHILDREN * pairs] = jnp.concatenate(tails, axis=0).astype(BF16)
    for j in range(kv_heads):
        for d in range(columns):
            out_ref[j * columns + d] = item[j]


def back_kernel(columns, in_ref, out_ref):
    pairs = out_ref.shape[1] - 1
    rows = pairs * PAIR
    mine = lax.axis_index("x")
    children = []
    for i in range(in_ref.shape[0]):
        tail = in_ref[i, CHILDREN * pairs].astype(F32)
        children.append([whole_number(tail[c : c + 1], 3 * rows) for c in range(CHILDREN)])
    for i in range(in_ref.shape[0]):
        for c in range(CHILDREN):
            child = children[i][c]

            @pl.when((child >= 0) & (child % columns == mine))
            def _():
                row = child // columns
                out_ref[row, :pairs] = in_ref[i, c * pairs : (c + 1) * pairs]
                tail = in_ref[i, CHILDREN * pairs].astype(F32)[c : c + 1]
                out_ref[row, pairs] = jnp.broadcast_to(tail, (PAIR, HD)).astype(BF16)


def merge_kernel(
    columns, facts_ref, in_ref, q_ref, nk_ref, nv_ref, rw_ref, out_ref, reward_ref, spare_ref, wide, came
):
    pairs = in_ref.shape[1] - 1
    rows = pairs * PAIR
    steps, heads = q_ref.shape[1], q_ref.shape[2] // HD
    kv_heads = nk_ref.shape[2] // HD
    size = steps * heads
    first = whole_number(facts_ref[0:1, :], 0) // (columns * kv_heads) * kv_heads
    lane = lax.broadcasted_iota(jnp.int32, (rows, HD), 1)
    own = lane % rows == lax.broadcasted_iota(jnp.int32, (rows, HD), 0)
    own = own & (lane < 3 * rows)
    tops = []
    for j in range(kv_heads):
        for g in range(pairs):
            came[j * rows + g * PAIR : j * rows + (g + 1) * PAIR, :] = in_ref[first + j, g].astype(F32)
        tail = in_ref[first + j, pairs].astype(F32)[0:1]
        tops.append(jnp.sum(jnp.where(own, tail, 0.0), axis=-1, keepdims=True))
        if j == 0:
            base = 3 * rows + 1
            inherited = (tail[:, base : base + 1] + tail[:, base + 1 : base + 2]) + tail[:, base + 2 : base + 3]
            spare_ref[...] = jnp.broadcast_to(inherited, spare_ref.shape)
    sum_parent = came[...]
    top_parent = jnp.concatenate(tops, axis=0)
    for h in range(heads):
        wide[h * steps : (h + 1) * steps, :] = q_ref[0, :, h * HD : (h + 1) * HD].astype(F32)
    query = wide[...]
    step = lax.broadcasted_iota(jnp.int32, (size, 1), 0) % steps

    def spread(ref, u):
        return jnp.concatenate(
            [
                jnp.broadcast_to(ref[0, u : u + 1, k * HD : (k + 1) * HD].astype(F32), (rows, HD))
                for k in range(kv_heads)
            ],
            axis=0,
        )

    scale = HD**-0.5
    logits = [
        jnp.where(u <= step, jnp.sum(query * spread(nk_ref, u), axis=-1, keepdims=True) * scale, -1e30)
        for u in range(steps)
    ]
    top_own = functools.reduce(jnp.maximum, logits)
    weights = [jnp.exp(x - top_own) for x in logits]
    total_own = functools.reduce(jnp.add, weights)
    sum_own = functools.reduce(
        jnp.add, [w.astype(BF16).astype(F32) * spread(nv_ref, u) for u, w in enumerate(weights)]
    )
    top = jnp.maximum(top_parent, top_own)
    factor_parent = jnp.exp(top_parent - top)
    factor_own = jnp.exp(top_own - top)
    merged = (sum_parent * factor_parent + sum_own * factor_own) / (
        factor_parent + total_own * factor_own
    )
    attended = merged.astype(BF16).astype(F32)
    wide[...] = attended
    reward = jnp.zeros((steps, HD), F32)
    for h in range(heads):
        part = wide[h * steps : (h + 1) * steps, :]
        out_ref[0, :, h * HD : (h + 1) * HD] = part.astype(BF16)
        reward = reward + part * rw_ref[h * HD : (h + 1) * HD].astype(F32)[None, :]
    reward_ref[...] = jnp.broadcast_to(jnp.sum(reward, axis=-1, keepdims=True), reward_ref.shape)


def per_device(
    cache_keys,
    cache_values,
    lengths,
    parent_scores,
    parents,
    queries,
    new_keys,
    new_values,
    reward_weight,
):
    columns = lax.axis_size("x")
    near, far = lax.axis_size(NEAR), lax.axis_size(FAR)
    steps, width = queries.shape[1:]
    heads = width // HD
    kv_heads = cache_keys.shape[2] // HD
    size = steps * heads
    rows = size // kv_heads
    pairs = rows // PAIR
    one, both = (pairs + 1, PAIR, HD), (CHILDREN * pairs + 1, PAIR, HD)

    def array(*shape, kind=BF16):
        return jax.ShapeDtypeStruct(shape, kind)

    sent, facts = pl.pallas_call(
        functools.partial(send_kernel, kv_heads),
        out_shape=(array(far, *one), array(TILE, HD, kind=F32)),
        in_specs=[SMEM, SMEM, SMEM, VMEM],
        out_specs=(VMEM, VMEM),
        compiler_params=limit(4),
        cost_estimate=SLOW,
        name="send",
    )(parents, lengths, parent_scores, queries)
    pieces = lax.all_to_all(sent, FAR, 0, 0, tiled=True)
    turned = pl.pallas_call(
        functools.partial(turn_kernel, columns),
        out_shape=array(near, *both),
        in_specs=[VMEM],
        out_specs=VMEM,
        scratch_shapes=[pltpu.SMEM((near,), jnp.int32), pltpu.VMEM((near, TILE, HD), F32)],
        compiler_params=limit(4),
        cost_estimate=SLOW,
        name="turn",
    )(pieces)
    asked = lax.all_to_all(turned, NEAR, 0, 0, tiled=True)
    outputs = pl.pallas_call(
        attend_kernel,
        out_shape=array(near, *both),
        in_specs=[VMEM, VMEM, VMEM, VMEM],
        out_specs=VMEM,
        scratch_shapes=[
            pltpu.VMEM((kv_heads, CHILDREN, rows, HD), F32),
            pltpu.VMEM((CHILDREN * rows, HD), F32),
            pltpu.VMEM((kv_heads, *both), BF16),
            pltpu.SMEM((1 + CHILDREN,), jnp.int32),
        ],
        compiler_params=limit(16),
        name="attend",
    )(facts, asked, cache_keys, cache_values)
    answers = lax.all_to_all(outputs, NEAR, 0, 0, tiled=True)
    back = pl.pallas_call(
        functools.partial(back_kernel, columns),
        out_shape=array(far, *one),
        in_specs=[VMEM],
        out_specs=VMEM,
        compiler_params=limit(4),
        name="back",
    )(answers)
    pieces = lax.all_to_all(back, FAR, 0, 0, tiled=True)
    output, partial_reward, inherited = pl.pallas_call(
        functools.partial(merge_kernel, columns),
        out_shape=(
            array(*queries.shape),
            array(steps, HD, kind=F32),
            array(1, HD, kind=F32),
        ),
        in_specs=[VMEM, VMEM, VMEM, VMEM, VMEM, VMEM],
        out_specs=(VMEM, VMEM, VMEM),
        scratch_shapes=[pltpu.VMEM((size, HD), F32), pltpu.VMEM((size, HD), F32)],
        compiler_params=limit(4),
        name="merge",
    )(facts, pieces, queries, new_keys, new_values, reward_weight)
    reward = lax.psum(partial_reward, "tensor")[:, 0]
    score = inherited[0, :1] + jnp.sum(jax.nn.log_sigmoid(reward))
    return (output, score)


def solution(mesh):
    finer = Mesh(
        mesh.devices.reshape(mesh.shape["groups"], 4, 4, 8, mesh.shape["tensor"]),
        ("groups", "zh", "zl", "x", "tensor"),
    )
    return jax.shard_map(
        per_device,
        mesh=finer,
        in_specs=(
            P(GROUPS_DP, None, "tensor"),
            P(GROUPS_DP, None, "tensor"),
            P(GROUPS_DP),
            P(GROUPS_DP),
            P(GROUPS_DP),
            P(GROUPS_DP, None, "tensor"),
            P(GROUPS_DP, None, "tensor"),
            P(GROUPS_DP, None, "tensor"),
            P("tensor"),
        ),
        out_specs=(P(GROUPS_DP, None, "tensor"), P(GROUPS_DP)),
        check_vma=False,
    )
```

```python
import functools

import jax
import jax.numpy as jnp
from jax import lax
from jax.experimental import pallas as pl
from jax.experimental.pallas import tpu as pltpu
from jax.sharding import Mesh
from jax.sharding import PartitionSpec as P

HD = 128
CHILDREN = 2
PAIR = 2
TILE = 8
GROUPS_DP = ("groups", "zh", "zl", "x")
NEAR = ("zl", "x")
FAR = ("zh", "zl")
VMEM = pl.BlockSpec(memory_space=pltpu.VMEM)
SMEM = pl.BlockSpec(memory_space=pltpu.SMEM)
BF16 = jnp.bfloat16
F32 = jnp.float32
SLOW = pl.CostEstimate(flops=10**11, bytes_accessed=2**28, transcendentals=0)


def limit(mib):
    return pltpu.CompilerParams(vmem_limit_bytes=mib * 1024 * 1024)


def whole_number(row, lane):
    return jnp.sum(row[:, lane : lane + 1]).astype(jnp.int32)


def in_parts(x):
    first = x.astype(BF16)
    rest = x - first.astype(F32)
    second = rest.astype(BF16)
    third = (rest - second.astype(F32)).astype(BF16)
    return [part.astype(F32) for part in (first, second, third)]


def facts_kernel(parents_ref, lengths_ref, scores_ref, facts_ref):
    facts = [parents_ref[0].astype(F32), lengths_ref[0].astype(F32), scores_ref[0]]
    for n, fact in enumerate(facts):
        facts_ref[n : n + 1, :] = jnp.full((1, HD), fact, F32)


def send_kernel(columns, parents_ref, q_ref, out_ref):
    steps = q_ref.shape[1]
    pairs = out_ref.shape[1] - 1
    turns = steps // PAIR
    parent = jnp.full((PAIR, HD), parents_ref[0].astype(F32), F32).astype(BF16)
    for j in range(out_ref.shape[0] // columns):
        for g in range(pairs):
            h, t = j * (pairs // turns) + g // turns, g % turns * PAIR
            pair = q_ref[0, t : t + PAIR, h * HD : (h + 1) * HD]
            for d in range(columns):
                out_ref[j * columns + d, g] = pair
        for d in range(columns):
            out_ref[j * columns + d, pairs] = parent


def turn_kernel(columns, in_ref, out_ref, used, meta):
    pairs = in_ref.shape[1] - 1
    block = in_ref.shape[0] // columns
    first = lax.axis_index("zh") * block
    mine = lax.axis_index("x")
    parents = [whole_number(in_ref[i, pairs].astype(F32)[0:1], 0) for i in range(in_ref.shape[0])]
    meta[...] = jnp.full(meta.shape, -1.0, F32)
    for i in range(out_ref.shape[0]):
        used[i] = 0
    for i, parent in enumerate(parents):

        @pl.when(parent % columns == mine)
        def _():
            row = parent // columns
            place = used[row]
            used[row] = place + 1
            out_ref[row, pl.ds(place * pairs, pairs)] = in_ref[i, :pairs]
            child = first * columns + i
            meta[row, pl.ds(place, 1), :] = jnp.full((1, HD), child.astype(F32), F32)

    for i in range(out_ref.shape[0]):
        out_ref[i, CHILDREN * pairs] = meta[i, :CHILDREN, :].astype(BF16)


def attend_kernel(facts_ref, in_ref, k_ref, v_ref, out_ref, q, result, item, found):
    kv_heads = item.shape[0]
    pairs = in_ref.shape[1] // CHILDREN
    rows = pairs * PAIR
    context = k_ref.shape[1]
    blocks = in_ref.shape[0] // kv_heads
    ids = []
    for b in range(blocks):
        tail = in_ref[b * kv_heads, CHILDREN * pairs].astype(F32)
        ids.append([whole_number(tail[c : c + 1], 0) for c in range(CHILDREN)])
    q[...] = jnp.zeros_like(q)
    found[0] = 0
    for c in range(CHILDREN):
        found[1 + c] = -1
    for b in range(blocks):
        for c in range(CHILDREN):

            @pl.when(ids[b][c] >= 0)
            def _():
                n = found[0]
                found[0] = n + 1
                found[1 + n] = ids[b][c]
                for j in range(kv_heads):
                    for g in range(pairs):
                        pair = in_ref[b * kv_heads + j, c * pairs + g].astype(F32)
                        q[j, n, g * PAIR : (g + 1) * PAIR, :] = pair

    scale = HD**-0.5
    length = facts_ref[1:2, 0:1].astype(jnp.int32)
    valid = lax.broadcasted_iota(jnp.int32, (CHILDREN * rows, context), 1) < length
    lane = lax.broadcasted_iota(jnp.int32, (rows, HD), 1)
    diagonal = lane % rows == lax.broadcasted_iota(jnp.int32, (rows, HD), 0)
    part = lax.broadcasted_iota(jnp.int32, (1, HD), 1)
    score = in_parts(facts_ref[2:3, :])
    for j in range(kv_heads):
        keys = k_ref[0, :, j * HD : (j + 1) * HD]
        values = v_ref[0, :, j * HD : (j + 1) * HD]
        query = q[j].reshape(CHILDREN * rows, HD).astype(BF16)
        logits = (
            lax.dot_general(query, keys, (((1,), (1,)), ((), ())), preferred_element_type=F32)
            * scale
        )
        logits = jnp.where(valid, logits, -1e30)
        top = jnp.max(logits, axis=-1, keepdims=True)
        weights = jnp.exp(logits - top)
        total = jnp.sum(weights, axis=-1, keepdims=True)
        summed = jnp.dot(weights.astype(BF16), values, preferred_element_type=F32)
        result[...] = summed / total
        for g in range(CHILDREN * pairs):
            item[j, g] = result[g * PAIR : (g + 1) * PAIR, :].astype(BF16)
        log_total = top + jnp.log(total)
        tails = []
        for c in range(CHILDREN):
            parts = in_parts(jnp.broadcast_to(log_total[c * rows : (c + 1) * rows], (rows, HD)))
            chosen = jnp.where(
                lane < rows, parts[0], jnp.where(lane < 2 * rows, parts[1], parts[2])
            )
            line = jnp.sum(jnp.where(diagonal, chosen, 0.0), axis=0, keepdims=True)
            for n, extra in enumerate([jnp.full((1, HD), found[1 + c].astype(F32), F32), *score]):
                line = jnp.where(part == 3 * rows + n, extra, line)
            tails.append(line)
        item[j, CHILDREN * pairs] = jnp.concatenate(tails, axis=0).astype(BF16)
    for b in range(blocks):
        out_ref[b * kv_heads : (b + 1) * kv_heads] = item[...]


def back_kernel(columns, in_ref, out_ref):
    pairs = out_ref.shape[1] - 1
    rows = pairs * PAIR
    first = lax.axis_index("zh") * out_ref.shape[0]
    children = []
    for i in range(in_ref.shape[0]):
        tail = in_ref[i, CHILDREN * pairs].astype(F32)
        children.append([whole_number(tail[c : c + 1], 3 * rows) for c in range(CHILDREN)])
    for i in range(in_ref.shape[0]):
        for c in range(CHILDREN):
            place = children[i][c] - first

            @pl.when((place >= 0) & (place < out_ref.shape[0]))
            def _():
                out_ref[place, :pairs] = in_ref[i, c * pairs : (c + 1) * pairs]
                tail = in_ref[i, CHILDREN * pairs].astype(F32)[c : c + 1]
                out_ref[place, pairs] = jnp.broadcast_to(tail, (PAIR, HD)).astype(BF16)


def merge_kernel(
    columns, facts_ref, in_ref, q_ref, nk_ref, nv_ref, rw_ref, out_ref, reward_ref, spare_ref, wide, came
):
    pairs = in_ref.shape[1] - 1
    rows = pairs * PAIR
    steps, heads = q_ref.shape[1], q_ref.shape[2] // HD
    kv_heads = nk_ref.shape[2] // HD
    size = steps * heads
    column = whole_number(facts_ref[0:1, :], 0) % columns
    lane = lax.broadcasted_iota(jnp.int32, (rows, HD), 1)
    own = lane % rows == lax.broadcasted_iota(jnp.int32, (rows, HD), 0)
    own = own & (lane < 3 * rows)
    tops = []
    for j in range(kv_heads):
        for g in range(pairs):
            came[j * rows + g * PAIR : j * rows + (g + 1) * PAIR, :] = in_ref[j * columns + column, g].astype(F32)
        tail = in_ref[j * columns + column, pairs].astype(F32)[0:1]
        tops.append(jnp.sum(jnp.where(own, tail, 0.0), axis=-1, keepdims=True))
        if j == 0:
            base = 3 * rows + 1
            inherited = (tail[:, base : base + 1] + tail[:, base + 1 : base + 2]) + tail[:, base + 2 : base + 3]
            spare_ref[...] = jnp.broadcast_to(inherited, spare_ref.shape)
    sum_parent = came[...]
    top_parent = jnp.concatenate(tops, axis=0)
    for h in range(heads):
        wide[h * steps : (h + 1) * steps, :] = q_ref[0, :, h * HD : (h + 1) * HD].astype(F32)
    query = wide[...]
    step = lax.broadcasted_iota(jnp.int32, (size, 1), 0) % steps

    def spread(ref, u):
        return jnp.concatenate(
            [
                jnp.broadcast_to(ref[0, u : u + 1, k * HD : (k + 1) * HD].astype(F32), (rows, HD))
                for k in range(kv_heads)
            ],
            axis=0,
        )

    scale = HD**-0.5
    logits = [
        jnp.where(u <= step, jnp.sum(query * spread(nk_ref, u), axis=-1, keepdims=True) * scale, -1e30)
        for u in range(steps)
    ]
    top_own = functools.reduce(jnp.maximum, logits)
    weights = [jnp.exp(x - top_own) for x in logits]
    total_own = functools.reduce(jnp.add, weights)
    sum_own = functools.reduce(
        jnp.add, [w.astype(BF16).astype(F32) * spread(nv_ref, u) for u, w in enumerate(weights)]
    )
    top = jnp.maximum(top_parent, top_own)
    factor_parent = jnp.exp(top_parent - top)
    factor_own = jnp.exp(top_own - top)
    merged = (sum_parent * factor_parent + sum_own * factor_own) / (
        factor_parent + total_own * factor_own
    )
    attended = merged.astype(BF16).astype(F32)
    wide[...] = attended
    reward = jnp.zeros((steps, HD), F32)
    for h in range(heads):
        part = wide[h * steps : (h + 1) * steps, :]
        out_ref[0, :, h * HD : (h + 1) * HD] = part.astype(BF16)
        reward = reward + part * rw_ref[h * HD : (h + 1) * HD].astype(F32)[None, :]
    reward_ref[...] = jnp.broadcast_to(jnp.sum(reward, axis=-1, keepdims=True), reward_ref.shape)


def per_device(
    cache_keys,
    cache_values,
    lengths,
    parent_scores,
    parents,
    queries,
    new_keys,
    new_values,
    reward_weight,
):
    columns = lax.axis_size("x")
    near, far = lax.axis_size(NEAR), lax.axis_size(FAR)
    steps, width = queries.shape[1:]
    heads = width // HD
    kv_heads = cache_keys.shape[2] // HD
    size = steps * heads
    rows = size // kv_heads
    pairs = rows // PAIR
    one, both = (pairs + 1, PAIR, HD), (CHILDREN * pairs + 1, PAIR, HD)

    def array(*shape, kind=BF16):
        return jax.ShapeDtypeStruct(shape, kind)

    sent = pl.pallas_call(
        functools.partial(send_kernel, columns),
        out_shape=array(near, *one),
        in_specs=[SMEM, VMEM],
        out_specs=VMEM,
        compiler_params=limit(4),
        cost_estimate=SLOW,
        name="send",
    )(parents, queries)
    facts = pl.pallas_call(
        facts_kernel,
        out_shape=array(TILE, HD, kind=F32),
        in_specs=[SMEM, SMEM, SMEM],
        out_specs=VMEM,
        compiler_params=limit(4),
        cost_estimate=SLOW,
        name="facts",
    )(parents, lengths, parent_scores)
    pieces = lax.all_to_all(sent, NEAR, 0, 0, tiled=True)
    turned = pl.pallas_call(
        functools.partial(turn_kernel, columns),
        out_shape=array(far, *both),
        in_specs=[VMEM],
        out_specs=VMEM,
        scratch_shapes=[pltpu.SMEM((far,), jnp.int32), pltpu.VMEM((far, TILE, HD), F32)],
        compiler_params=limit(4),
        cost_estimate=SLOW,
        name="turn",
    )(pieces)
    asked = lax.all_to_all(turned, FAR, 0, 0, tiled=True)
    outputs = pl.pallas_call(
        attend_kernel,
        out_shape=array(far, *both),
        in_specs=[VMEM, VMEM, VMEM, VMEM],
        out_specs=VMEM,
        scratch_shapes=[
            pltpu.VMEM((kv_heads, CHILDREN, rows, HD), F32),
            pltpu.VMEM((CHILDREN * rows, HD), F32),
            pltpu.VMEM((kv_heads, *both), BF16),
            pltpu.SMEM((1 + CHILDREN,), jnp.int32),
        ],
        compiler_params=limit(16),
        name="attend",
    )(facts, asked, cache_keys, cache_values)
    answers = lax.all_to_all(outputs, FAR, 0, 0, tiled=True)
    back = pl.pallas_call(
        functools.partial(back_kernel, columns),
        out_shape=array(near, *one),
        in_specs=[VMEM],
        out_specs=VMEM,
        compiler_params=limit(4),
        name="back",
    )(answers)
    pieces = lax.all_to_all(back, NEAR, 0, 0, tiled=True)
    output, partial_reward, inherited = pl.pallas_call(
        functools.partial(merge_kernel, columns),
        out_shape=(
            array(*queries.shape),
            array(steps, HD, kind=F32),
            array(1, HD, kind=F32),
        ),
        in_specs=[VMEM, VMEM, VMEM, VMEM, VMEM, VMEM],
        out_specs=(VMEM, VMEM, VMEM),
        scratch_shapes=[pltpu.VMEM((size, HD), F32), pltpu.VMEM((size, HD), F32)],
        compiler_params=limit(4),
        name="merge",
    )(facts, pieces, queries, new_keys, new_values, reward_weight)
    reward = lax.psum(partial_reward, "tensor")[:, 0]
    score = inherited[0, :1] + jnp.sum(jax.nn.log_sigmoid(reward))
    return (output, score)


def solution(mesh):
    finer = Mesh(
        mesh.devices.reshape(mesh.shape["groups"], 4, 4, 8, mesh.shape["tensor"]),
        ("groups", "zh", "zl", "x", "tensor"),
    )
    return jax.shard_map(
        per_device,
        mesh=finer,
        in_specs=(
            P(GROUPS_DP, None, "tensor"),
            P(GROUPS_DP, None, "tensor"),
            P(GROUPS_DP),
            P(GROUPS_DP),
            P(GROUPS_DP),
            P(GROUPS_DP, None, "tensor"),
            P(GROUPS_DP, None, "tensor"),
            P(GROUPS_DP, None, "tensor"),
            P("tensor"),
        ),
        out_specs=(P(GROUPS_DP, None, "tensor"), P(GROUPS_DP)),
        check_vma=False,
    )
```
